32 devices in a mesh: tab: 2 (over x), cand: 4 (over z), dp: 4 (over y, core).
Axes of the slice: x: 2, y: 2, z: 4, core: 2. Of those that a mesh axis runs over, the one named last changes fastest.
Arguments:
- tables: bfloat16 [16, 65536, 128], P(('cand', 'dp'), 'tab'), may hold values from -6 to 6
- bag_ids: int32 [16, 1024, 16], P(('cand', 'dp')), may hold values from 0 to 65535
- bag_lengths: int32 [16, 1024], P(('cand', 'dp')), may hold values from 1 to 16
- item_weight: bfloat16 [2048, 256], replicated, may hold values from -0.125 to 0.125
- user_features: bfloat16 [16384, 512], P(('tab', 'dp')), may hold values from -6 to 6
- user_w1: bfloat16 [512, 1024], replicated, may hold values from -0.25 to 0.25
- user_w2: bfloat16 [1024, 256], replicated, may hold values from -0.1875 to 0.1875
- positive_items: int32 [16384], P(('tab', 'dp')), may hold values from 0 to 1023
Outputs:
- item_emb: float32 [1024, 256], P(('tab', 'cand', 'dp'))
- user_loss: float32 [16384], P(('tab', 'dp'))
The draws below stay inside these ranges and needn't reach their ends.
Inputs may be any that keep to these rules, and one draw needn't show every extreme that they name: `bag_ids`: row ids of a table. Only the first bag_lengths ids of a bag count; the rest is padding.
All inputs are finite; a program needn't handle non-finite values.
Results may differ from the reference program's by a relative error of at most 0.00046.
Values sent between devices are 32-bit elements; how exact they have to be, the bound alone decides.
A program may use at most 64 MiB of HBM per device.

```python
import jax
import jax.numpy as jnp
from jax import lax

E = 128
H = 256
DU = 512
HU = 1024
L = 16
ITEMS = 1024
F = 16
VOCAB = 65536
USERS = 16384


def place_ends(array, stream_key, least, top_value):
    place = [jax.random.randint(jax.random.fold_in(stream_key, axis), (), 0, length) for axis, length in enumerate(array.shape)]
    main_axis = array.shape.index(max(array.shape))
    next_to = place[:main_axis] + [(place[main_axis] + 1) % array.shape[main_axis]] + place[main_axis + 1:]
    return array.at[tuple(place)].set(least).at[tuple(next_to)].set(top_value)


def levels(own_key, shape, pieces, least, largest):
    factor_of, own = 1.0, jax.random.fold_in(own_key, 6)
    for position, parts in pieces:
        heights = jnp.exp(jax.random.uniform(jax.random.fold_in(own, position), (parts,), jnp.float32, least / len(pieces), largest / len(pieces)))
        factor_of = factor_of * jnp.repeat(heights, shape[position] // parts).reshape([-1 if axis == position else 1 for axis in range(len(shape))])
    return factor_of


def noise(stream_key, extent, spread, limit, split=(), held_as=jnp.bfloat16):
    gain = levels(stream_key, extent, split, -0.22, 0.18) if split else 1.0
    result = jax.random.normal(stream_key, extent, jnp.float32) * spread * gain
    return jnp.minimum(jnp.maximum(result, -limit), limit).astype(held_as)


def setup_inputs(seed: int = 0) -> dict:
    splits = jax.random.split(jax.random.key(seed), 9)
    return {
        "tables": noise(splits[0], (F, VOCAB, E), 1.0, 6.0, ((0, 16), (1, 2))),
        "bag_ids": place_ends(jax.random.randint(splits[1], (F, ITEMS, L), 0, VOCAB), jax.random.fold_in(splits[1], 1), 0, VOCAB - 1).astype(jnp.int32),
        "bag_lengths": place_ends(jax.random.randint(splits[2], (F, ITEMS), 1, L + 1), jax.random.fold_in(splits[2], 1), 1, L).astype(jnp.int32),
        "item_weight": noise(splits[3], (F * E, H), (F * E) ** -0.5, 0.125),
        "user_features": noise(splits[4], (USERS, DU), 1.0, 6.0, ((0, 8),)),
        "user_w1": noise(splits[5], (DU, HU), DU ** -0.5, 0.25),
        "user_w2": noise(splits[6], (HU, H), HU ** -0.5, 0.1875),
        "positive_items": place_ends(jax.random.randint(splits[7], (USERS,), 0, ITEMS), jax.random.fold_in(splits[7], 1), 0, ITEMS - 1).astype(jnp.int32),
    }


epsilon = 1e-06
logit_scale = 20.0

def unit_rows(vectors):
    return vectors * lax.rsqrt(lax.optimization_barrier(jnp.mean(vectors * vectors, axis=-1, keepdims=True)) + epsilon)

def pool_table(inputs):
    table, bag_ids, lengths = inputs
    gathered = jnp.take(table, bag_ids, axis=0).astype(jnp.float32)
    valid = lax.broadcasted_iota(jnp.int32, bag_ids.shape, 1) < lengths[:, None]
    summed = lax.optimization_barrier(jnp.sum(jnp.where(valid[:, :, None], gathered, jnp.float32(0.0)), axis=1))
    return summed / lengths[:, None].astype(jnp.float32)

def reference(tables, bag_ids, bag_lengths, item_weight, user_features, user_w1, user_w2, positive_items):
    pooled = lax.map(pool_table, (tables, bag_ids, bag_lengths))
    joined = jnp.transpose(pooled, (1, 0, 2)).reshape(ITEMS, F * E)
    item_pre = jnp.dot(joined, item_weight.astype(jnp.float32), precision=lax.Precision.HIGHEST, preferred_element_type=jnp.float32)
    item_emb = unit_rows(item_pre)
    user_hidden = jax.nn.gelu(jnp.dot(user_features, user_w1, preferred_element_type=jnp.float32), approximate=False).astype(jnp.bfloat16)
    user_pre = jnp.dot(user_hidden, user_w2, preferred_element_type=jnp.float32)
    user_emb = unit_rows(user_pre)
    scores = jnp.dot(user_emb, item_emb.T, precision=lax.Precision.HIGHEST, preferred_element_type=jnp.float32) * (logit_scale / H)
    totals = lax.optimization_barrier(jnp.sum(jnp.exp(scores), axis=1))
    positive = jnp.take_along_axis(scores, positive_items[:, None].astype(jnp.int32), axis=1)[:, 0]
    user_loss = jnp.log(totals) - positive
    return (item_emb, user_loss)
```

```python
import functools
import math

import jax
import jax.numpy as jnp
from jax import lax
from jax.experimental import pallas as pl
from jax.experimental.pallas import tpu as pltpu
from jax.sharding import PartitionSpec as P

epsilon = 1e-06
logit_scale = 20.0
MESH = pl.DeviceIdType.MESH
F32 = jnp.float32
BF16 = jnp.bfloat16
VMEM_LIMIT = 60 * 1024 * 1024
LANES = 128
SUBLANES = 8
ZERO_ROWS = 32


def split2(x):
    hi = x.astype(BF16)
    return hi, (x - hi.astype(F32)).astype(BF16)


def unit_rows(vectors):
    return vectors * lax.rsqrt(jnp.mean(vectors * vectors, axis=-1, keepdims=True) + epsilon)


def dot(a, b):
    return jnp.dot(a, b, preferred_element_type=F32)


def run_step(
    sizes,
    ids_in,
    lengths_in,
    table,
    weight_in,
    features_in,
    w1_in,
    w2_in,
    positives_in,
    emb_out,
    loss_out,
    ids_raw,
    lengths,
    index_rows,
    inverse,
    narrow,
    wide,
    weight,
    features,
    w1,
    w2,
    positives,
    pooled,
    arrived,
    joined,
    emb,
    user_hi,
    user_lo,
    gathered,
    items_flat,
    sums_here,
    sums_all,
    loss,
    load_sems,
    table_sems,
    index_sems,
    out_sems,
    send_a,
    recv_a,
    send_b,
    recv_b,
    send_c,
    recv_c,
    *index,
):
    num_tab, num_cand, num_dp = sizes
    total = num_tab * num_cand * num_dp
    groups = num_cand * num_dp
    slots = num_tab * num_dp
    t, c, d = (lax.axis_index(n) for n in ("tab", "cand", "dp"))
    me = (t * num_cand + c) * num_dp + d
    my_slot = t * num_dp + d
    per_block, width = pooled.shape[1:]
    items = total * per_block
    length = ids_raw.shape[0]
    rows, _ = table.shape
    users = features.shape[0]
    hidden = w1.shape[1]
    embed = w2.shape[1]
    chunks = table_sems.shape[0]
    chunk = rows // chunks
    held = narrow.shape[0]
    blocks_step = max(1, 32 // per_block)
    steps = total // blocks_step
    items_step = items // steps
    columns = items // LANES

    def place(index):
        return (index // groups, index // num_dp % num_cand, index % num_dp)

    barrier = pltpu.get_barrier_semaphore()

    loads = [
        pltpu.make_async_copy(a, b, load_sems.at[i])
        for i, (a, b) in enumerate(
            (
                (ids_in, ids_raw),
                (lengths_in, lengths),
                (w1_in, w1),
                (w2_in, w2),
                (features_in, features),
                (weight_in, weight),
                (positives_in, positives),
            )
        )
    ]

    def chunk_copy(n):
        part = pl.ds(pl.multiple_of(n * chunk, chunk), chunk)
        return pltpu.make_async_copy(table.at[part], narrow.at[lax.rem(n, held)], table_sems.at[n])

    for load in loads[:2]:
        load.start()
    for n in range(min(chunks, held)):
        chunk_copy(n).start()
    for load in loads[2:]:
        load.start()

    @pl.loop(1, total)
    def _(j):
        peer = lax.rem(me + j, total)
        pl.semaphore_signal(barrier, inc=1, device_id=place(peer), device_id_type=MESH)

    wide[pl.ds(rows, ZERO_ROWS), :] = jnp.zeros((ZERO_ROWS, width), F32)
    for load in loads[:2]:
        load.wait()
    first_row = t * rows
    spread = lax.broadcasted_iota(jnp.int32, (SUBLANES, LANES), 1) % 2 * (ZERO_ROWS // 2)
    line = lax.broadcasted_iota(jnp.int32, (SUBLANES, LANES), 0)
    for b in range(columns):
        lanes = slice(b * LANES, (b + 1) * LANES)
        count = lengths[:, lanes]
        for p in range(0, length, SUBLANES):
            local = ids_raw[p : p + SUBLANES, lanes] - first_row
            position = line + p
            keeping = (local >= 0) & (local < rows) & (position < count)
            spare = rows + position % (ZERO_ROWS // 2) + spread
            index_rows[p : p + SUBLANES, lanes] = jnp.where(keeping, local, spare)
    index_copies = [
        pltpu.make_async_copy(index_rows.at[p], index[p], index_sems.at[p]) for p in range(length)
    ]
    for copy in index_copies:
        copy.start()
    for b in range(columns):
        lanes = slice(b * LANES, (b + 1) * LANES)
        scale = 1.0 / lengths[:, lanes].astype(F32)
        inverse[lanes, :] = jnp.broadcast_to(scale, (LANES, LANES)).T

    @pl.loop(0, chunks)
    def _(n):
        chunk_copy(n).wait()
        part = pl.ds(pl.multiple_of(n * chunk, chunk), chunk)
        wide[part, :] = narrow[lax.rem(n, held)].astype(F32)
        if held < chunks:

            @pl.when(n + held < chunks)
            def _():
                chunk_copy(n + held).start()

    for copy in index_copies:
        copy.wait()
    pl.semaphore_wait(barrier, total - 1)

    def send(dest):
        pltpu.make_async_remote_copy(
            src_ref=pooled.at[dest],
            dst_ref=arrived.at[me],
            send_sem=send_a,
            recv_sem=recv_a,
            device_id=place(dest),
            device_id_type=MESH,
        ).start()

    def group_at(s):
        if blocks_step > 1 or num_cand != 4:
            return lax.rem(me // blocks_step + 1 + s, steps)
        turn = s // slots
        plane = jnp.where(
            turn == 0,
            (c + 2) % 4,
            jnp.where(turn == 1, 3 - c, jnp.where(turn == 2, c + 1 - c % 2 * 2, c)),
        )
        slot = lax.rem(my_slot + 1 + s, slots)
        return (slot // num_dp * num_cand + plane) * num_dp + slot % num_dp

    @pl.loop(0, steps)
    def _(s):
        @pl.when(s > 0)
        def _():
            before = group_at(s - 1)
            for i in range(blocks_step):
                send(before * blocks_step + i)

        group = group_at(s)
        first = group * items_step
        for k in range(items_step):
            terms = [wide[pl.ds(of_place[first + k], 1), :] for of_place in index]
            while len(terms) > 1:
                terms = [a + b for a, b in zip(terms[::2], terms[1::2])] + (
                    [terms[-1]] if len(terms) % 2 else []
                )
            row = terms[0] * inverse[pl.ds(first + k, 1), :]
            pooled[group * blocks_step + k // per_block, pl.ds(k % per_block, 1), :] = row

    last = group_at(steps - 1)
    for i in range(blocks_step):
        dest = last * blocks_step + i
        if blocks_step > 1:

            @pl.when(dest != me)
            def _():
                send(dest)

    for load in loads[2:]:
        load.wait()
    tile = min(users, TILE)
    part_width = min(hidden, 256)

    @pl.loop(0, users // tile)
    def _(n):
        user_rows = pl.ds(pl.multiple_of(n * tile, tile), tile)
        x = features[user_rows, :]
        pre = None
        for h in range(0, hidden, part_width):
            z = dot(x, w1[:, h : h + part_width])
            z = z * (0.5 * lax.erf(z * math.sqrt(0.5)) + 0.5)
            term = dot(z.astype(BF16), w2[h : h + part_width, :])
            pre = term if pre is None else pre + term
        hi, lo = split2(unit_rows(pre) * (logit_scale / embed))
        user_hi[user_rows, :] = hi
        user_lo[user_rows, :] = lo

    arrived[me] = pooled[me]
    others = pl.ds(0, total - 1)
    pltpu.make_async_copy(arrived.at[others], arrived.at[others], recv_a).wait()
    for f in range(groups):
        block = arrived[f]
        for s in range(1, num_tab):
            block = block + arrived[s * groups + f]
        joined[:, f * width : (f + 1) * width] = block
    hi, lo = split2(joined[...])
    both = dot(jnp.concatenate([hi, lo], axis=0), weight[...])
    item_emb = unit_rows(both[:per_block] + both[per_block:])
    emb[...] = item_emb

    @pl.loop(1, slots)
    def _(j):
        slot = lax.rem(my_slot + j, slots)
        pltpu.make_async_remote_copy(
            src_ref=emb,
            dst_ref=gathered.at[my_slot],
            send_sem=send_b,
            recv_sem=recv_b,
            device_id=(slot // num_dp, c, lax.rem(slot, num_dp)),
            device_id_type=MESH,
        ).start()

    emb_copy = pltpu.make_async_copy(emb, emb_out, out_sems.at[0])
    emb_copy.start()
    gathered[my_slot] = item_emb
    others_b = pl.ds(0, slots - 1)
    pltpu.make_async_copy(gathered.at[others_b], gathered.at[others_b], recv_b).wait()
    for s in range(slots):
        items_flat[s * per_block : (s + 1) * per_block, :] = gathered[s]
    item_hi, item_lo = split2(items_flat[...])
    count = slots * per_block
    column = min(users, 256)

    @pl.loop(0, users // column)
    def _(u):
        rows = pl.ds(pl.multiple_of(u * column, column), column)
        uh, ul = user_hi[rows, :], user_lo[rows, :]

        def cross(a, b):
            return lax.dot_general(a, b, (((1,), (1,)), ((), ())), preferred_element_type=F32)

        scores = cross(item_lo, uh) + cross(item_hi, ul) + cross(item_hi, uh)
        line = lax.broadcasted_iota(jnp.int32, (count, 1), 0)
        slot = line // per_block
        ids = ((slot // num_dp * num_cand + c) * num_dp + slot % num_dp) * per_block + line % per_block
        sums_here[0:1, rows] = jnp.sum(jnp.exp(scores), axis=0, keepdims=True)
        sums_here[1:2, rows] = jnp.sum(
            jnp.where(ids == positives[:, rows], scores, jnp.float32(0.0)), axis=0, keepdims=True
        )

    @pl.loop(1, num_cand)
    def _(j):
        peer = lax.rem(c + j, num_cand)
        pltpu.make_async_remote_copy(
            src_ref=sums_here,
            dst_ref=sums_all.at[c],
            send_sem=send_c,
            recv_sem=recv_c,
            device_id=(t, peer, d),
            device_id_type=MESH,
        ).start()

    sums_all[c] = sums_here[...]
    others_c = pl.ds(0, num_cand - 1)
    pltpu.make_async_copy(sums_all.at[others_c], sums_all.at[others_c], recv_c).wait()
    both = sums_all[0]
    for s in range(1, num_cand):
        both = both + sums_all[s]
    loss[...] = jnp.log(both[0:1, :]) - both[1:2, :]
    loss_copy = pltpu.make_async_copy(loss, loss_out, out_sems.at[1])
    loss_copy.start()

    pltpu.make_async_copy(pooled.at[others], pooled.at[others], send_a).wait()
    pltpu.make_async_copy(gathered.at[others_b], gathered.at[others_b], send_b).wait()
    pltpu.make_async_copy(sums_all.at[others_c], sums_all.at[others_c], send_c).wait()
    emb_copy.wait()
    loss_copy.wait()


TILE = 256


def body(
    tables, bag_ids, bag_lengths, item_weight, user_features, user_w1, user_w2, positive_items
):
    sizes = tuple(lax.axis_size(n) for n in ("tab", "cand", "dp"))
    total = math.prod(sizes)
    slots = sizes[0] * sizes[2]
    table = tables[0]
    rows, width = table.shape
    items, length = bag_ids.shape[1:]
    per_block = items // total
    users = user_features.shape[0]
    embed = user_w2.shape[1]
    chunk = min(rows, 4096)
    chunks = rows // chunk
    held = min(chunks, 8)
    anywhere = pl.BlockSpec(memory_space=pl.ANY)
    item_emb, loss = pl.pallas_call(
        functools.partial(run_step, sizes),
        out_shape=(
            jax.ShapeDtypeStruct((per_block, embed), F32),
            jax.ShapeDtypeStruct((1, users), F32),
        ),
        in_specs=[anywhere] * 8,
        out_specs=(anywhere, anywhere),
        scratch_shapes=[
            pltpu.VMEM((length, items), jnp.int32),
            pltpu.VMEM((1, items), jnp.int32),
            pltpu.VMEM((length, items), jnp.int32),
            pltpu.VMEM((items, LANES), F32),
            pltpu.VMEM((held, chunk, width), BF16),
            pltpu.VMEM((rows + ZERO_ROWS, width), F32),
            pltpu.VMEM(item_weight.shape, BF16),
            pltpu.VMEM(user_features.shape, BF16),
            pltpu.VMEM(user_w1.shape, BF16),
            pltpu.VMEM(user_w2.shape, BF16),
            pltpu.VMEM((1, users), jnp.int32),
            pltpu.VMEM((total, per_block, width), F32),
            pltpu.VMEM((total, per_block, width), F32),
            pltpu.VMEM((per_block, item_weight.shape[0]), F32),
            pltpu.VMEM((per_block, embed), F32),
            pltpu.VMEM((users, embed), BF16),
            pltpu.VMEM((users, embed), BF16),
            pltpu.VMEM((slots, per_block, embed), F32),
            pltpu.VMEM((slots * per_block, embed), F32),
            pltpu.VMEM((2, users), F32),
            pltpu.VMEM((sizes[1], 2, users), F32),
            pltpu.VMEM((1, users), F32),
            pltpu.SemaphoreType.DMA((7,)),
            pltpu.SemaphoreType.DMA((chunks,)),
            pltpu.SemaphoreType.DMA((length,)),
            pltpu.SemaphoreType.DMA((2,)),
        ]
        + [pltpu.SemaphoreType.DMA] * 6
        + [pltpu.SMEM((items,), jnp.int32)] * length,
        compiler_params=pltpu.CompilerParams(
            collective_id=0, has_side_effects=True, vmem_limit_bytes=VMEM_LIMIT
        ),
        name="step",
    )(
        bag_ids[0].T,
        bag_lengths,
        table,
        item_weight,
        user_features,
        user_w1,
        user_w2,
        positive_items[None, :],
    )
    return (item_emb, loss[0])


def solution(mesh):
    placed = (
        P(("cand", "dp"), "tab", None),
        P(("cand", "dp"), None, None),
        P(("cand", "dp"), None),
        P(),
        P(("tab", "dp"), None),
        P(),
        P(),
        P(("tab", "dp")),
    )
    return jax.shard_map(
        body,
        mesh=mesh,
        in_specs=placed,
        out_specs=(P(("tab", "cand", "dp"), None), P(("tab", "dp"))),
        check_vma=False,
    )
```

```python
import functools
import math

import jax
import jax.numpy as jnp
from jax import lax
from jax.experimental import pallas as pl
from jax.experimental.pallas import tpu as pltpu
from jax.sharding import PartitionSpec as P

epsilon = 1e-06
logit_scale = 20.0
MESH = pl.DeviceIdType.MESH
F32 = jnp.float32
BF16 = jnp.bfloat16
VMEM_LIMIT = 60 * 1024 * 1024
LANES = 128
SUBLANES = 8
ZERO_ROWS = 32


def split2(x):
    hi = x.astype(BF16)
    return hi, (x - hi.astype(F32)).astype(BF16)


def unit_rows(vectors):
    return vectors * lax.rsqrt(jnp.mean(vectors * vectors, axis=-1, keepdims=True) + epsilon)


def dot(a, b):
    return jnp.dot(a, b, preferred_element_type=F32)


def run_step(
    sizes,
    ids_in,
    lengths_in,
    table,
    weight_in,
    features_in,
    w1_in,
    w2_in,
    positives_in,
    emb_out,
    loss_out,
    ids_raw,
    lengths,
    index_rows,
    inverse,
    narrow,
    wide,
    weight,
    features,
    w1,
    w2,
    positives,
    pooled,
    arrived,
    joined,
    emb,
    user_hi,
    user_lo,
    gathered,
    items_flat,
    sums_here,
    sums_all,
    loss,
    load_sems,
    table_sems,
    index_sems,
    out_sems,
    send_a,
    recv_a,
    send_b,
    recv_b,
    send_c,
    recv_c,
    ready,
    *index,
):
    num_tab, num_cand, num_dp = sizes
    total = num_tab * num_cand * num_dp
    groups = num_cand * num_dp
    slots = num_tab * num_dp
    t, c, d = (lax.axis_index(n) for n in ("tab", "cand", "dp"))
    me = (t * num_cand + c) * num_dp + d
    my_slot = t * num_dp + d
    per_block, width = pooled.shape[1:]
    items = total * per_block
    length = ids_raw.shape[0]
    rows, _ = table.shape
    users = features.shape[0]
    hidden = w1.shape[1]
    embed = w2.shape[1]
    chunks = table_sems.shape[0]
    chunk = rows // chunks
    held = narrow.shape[0]
    blocks_step = max(1, 32 // per_block)
    steps = total // blocks_step
    items_step = items // steps
    columns = items // LANES

    def place(index):
        return (index // groups, index // num_dp % num_cand, index % num_dp)

    barrier = pltpu.get_barrier_semaphore()

    loads = [
        pltpu.make_async_copy(a, b, load_sems.at[i])
        for i, (a, b) in enumerate(
            (
                (ids_in, ids_raw),
                (lengths_in, lengths),
                (w1_in, w1),
                (w2_in, w2),
                (features_in, features),
                (weight_in, weight),
                (positives_in, positives),
            )
        )
    ]

    def chunk_copy(n):
        part = pl.ds(pl.multiple_of(n * chunk, chunk), chunk)
        return pltpu.make_async_copy(table.at[part], narrow.at[lax.rem(n, held)], table_sems.at[n])

    def in_plane(slot):
        return (slot // num_dp, c, slot % num_dp)

    for load in loads[:2]:
        load.start()

    @pl.loop(1, num_cand)
    def _(j):
        peer = (t, lax.rem(c + j, num_cand), d)
        pl.semaphore_signal(barrier, inc=1, device_id=peer, device_id_type=MESH)

    @pl.loop(1, slots)
    def _(j):
        peer = in_plane(lax.rem(my_slot + j, slots))
        pl.semaphore_signal(barrier, inc=1, device_id=peer, device_id_type=MESH)

    for n in range(min(chunks, held)):
        chunk_copy(n).start()
    wide[pl.ds(rows, ZERO_ROWS), :] = jnp.zeros((ZERO_ROWS, width), F32)
    for load in loads[:2]:
        load.wait()
    first_row = t * rows
    spread = lax.broadcasted_iota(jnp.int32, (SUBLANES, LANES), 1) % 2 * (ZERO_ROWS // 2)
    line = lax.broadcasted_iota(jnp.int32, (SUBLANES, LANES), 0)
    for b in range(columns):
        lanes = slice(b * LANES, (b + 1) * LANES)
        count = lengths[:, lanes]
        for p in range(0, length, SUBLANES):
            local = ids_raw[p : p + SUBLANES, lanes] - first_row
            position = line + p
            keeping = (local >= 0) & (local < rows) & (position < count)
            spare = rows + position % (ZERO_ROWS // 2) + spread
            index_rows[p : p + SUBLANES, lanes] = jnp.where(keeping, local, spare)
    index_copies = [
        pltpu.make_async_copy(index_rows.at[p], index[p], index_sems.at[p]) for p in range(length)
    ]
    for copy in index_copies:
        copy.start()
    for b in range(columns):
        lanes = slice(b * LANES, (b + 1) * LANES)
        scale = 1.0 / lengths[:, lanes].astype(F32)
        inverse[lanes, :] = jnp.broadcast_to(scale, (LANES, LANES)).T

    pl.semaphore_wait(barrier, num_cand - 1 + slots - 1)

    @pl.loop(1, slots)
    def _(j):
        peer = in_plane(lax.rem(my_slot + j, slots))
        pl.semaphore_signal(ready, inc=1, device_id=peer, device_id_type=MESH)

    @pl.loop(0, chunks)
    def _(n):
        chunk_copy(n).wait()
        part = pl.ds(pl.multiple_of(n * chunk, chunk), chunk)
        wide[part, :] = narrow[lax.rem(n, held)].astype(F32)
        if held < chunks:

            @pl.when(n + held < chunks)
            def _():
                chunk_copy(n + held).start()

    for load in loads[2:]:
        load.start()
    for copy in index_copies:
        copy.wait()

    def send(dest):
        pltpu.make_async_remote_copy(
            src_ref=pooled.at[dest],
            dst_ref=arrived.at[me],
            send_sem=send_a,
            recv_sem=recv_a,
            device_id=place(dest),
            device_id_type=MESH,
        ).start()

    def group_at(s):
        if blocks_step > 1 or num_cand != 4:
            return lax.rem(me // blocks_step + 1 + s, steps)
        turn = s // slots
        plane = jnp.where(
            turn == 0,
            (c + 2) % 4,
            jnp.where(turn == 1, 3 - c, jnp.where(turn == 2, c + 1 - c % 2 * 2, c)),
        )
        slot = lax.rem(my_slot + 1 + s, slots)
        return (slot // num_dp * num_cand + plane) * num_dp + slot % num_dp

    @pl.loop(0, steps)
    def _(s):
        @pl.when(s == 1)
        def _():
            pl.semaphore_wait(ready, slots - 1)

        @pl.when(s > 0)
        def _():
            before = group_at(s - 1)
            for i in range(blocks_step):
                send(before * blocks_step + i)

        group = group_at(s)
        first = group * items_step
        for k in range(items_step):
            terms = [wide[pl.ds(of_place[first + k], 1), :] for of_place in index]
            while len(terms) > 1:
                terms = [a + b for a, b in zip(terms[::2], terms[1::2])] + (
                    [terms[-1]] if len(terms) % 2 else []
                )
            row = terms[0] * inverse[pl.ds(first + k, 1), :]
            pooled[group * blocks_step + k // per_block, pl.ds(k % per_block, 1), :] = row

    last = group_at(steps - 1)
    for i in range(blocks_step):
        dest = last * blocks_step + i
        if blocks_step > 1:

            @pl.when(dest != me)
            def _():
                send(dest)

    for load in loads[2:]:
        load.wait()
    tile = min(users, TILE)
    part_width = min(hidden, 256)

    def tower(n):
        user_rows = pl.ds(pl.multiple_of(n * tile, tile), tile)
        x = features[user_rows, :]
        pre = None
        for h in range(0, hidden, part_width):
            z = dot(x, w1[:, h : h + part_width])
            z = z * (0.5 * lax.erf(z * math.sqrt(0.5)) + 0.5)
            term = dot(z.astype(BF16), w2[h : h + part_width, :])
            pre = term if pre is None else pre + term
        hi, lo = split2(unit_rows(pre) * (logit_scale / embed))
        user_hi[user_rows, :] = hi
        user_lo[user_rows, :] = lo

    tiles = users // tile
    early = tiles * EARLY // 8
    pl.loop(0, early)(tower)

    arrived[me] = pooled[me]
    others = pl.ds(0, total - 1)
    pltpu.make_async_copy(arrived.at[others], arrived.at[others], recv_a).wait()
    for f in range(groups):
        block = arrived[f]
        for s in range(1, num_tab):
            block = block + arrived[s * groups + f]
        joined[:, f * width : (f + 1) * width] = block
    hi, lo = split2(joined[...])
    both = dot(jnp.concatenate([hi, lo], axis=0), weight[...])
    item_emb = unit_rows(both[:per_block] + both[per_block:])
    emb[...] = item_emb

    @pl.loop(1, slots)
    def _(j):
        slot = lax.rem(my_slot + j, slots)
        pltpu.make_async_remote_copy(
            src_ref=emb,
            dst_ref=gathered.at[my_slot],
            send_sem=send_b,
            recv_sem=recv_b,
            device_id=in_plane(slot),
            device_id_type=MESH,
        ).start()

    emb_copy = pltpu.make_async_copy(emb, emb_out, out_sems.at[0])
    emb_copy.start()
    gathered[my_slot] = item_emb
    pl.loop(early, tiles)(tower)
    others_b = pl.ds(0, slots - 1)
    pltpu.make_async_copy(gathered.at[others_b], gathered.at[others_b], recv_b).wait()
    for s in range(slots):
        items_flat[s * per_block : (s + 1) * per_block, :] = gathered[s]
    item_hi, item_lo = split2(items_flat[...])
    count = slots * per_block
    column = min(users, 256)

    @pl.loop(0, users // column)
    def _(u):
        rows = pl.ds(pl.multiple_of(u * column, column), column)
        uh, ul = user_hi[rows, :], user_lo[rows, :]

        def cross(a, b):
            return lax.dot_general(a, b, (((1,), (1,)), ((), ())), preferred_element_type=F32)

        scores = cross(item_lo, uh) + cross(item_hi, ul) + cross(item_hi, uh)
        line = lax.broadcasted_iota(jnp.int32, (count, 1), 0)
        slot = line // per_block
        ids = ((slot // num_dp * num_cand + c) * num_dp + slot % num_dp) * per_block + line % per_block
        sums_here[0:1, rows] = jnp.sum(jnp.exp(scores), axis=0, keepdims=True)
        sums_here[1:2, rows] = jnp.sum(
            jnp.where(ids == positives[:, rows], scores, jnp.float32(0.0)), axis=0, keepdims=True
        )

    @pl.loop(1, num_cand)
    def _(j):
        peer = lax.rem(c + j, num_cand)
        pltpu.make_async_remote_copy(
            src_ref=sums_here,
            dst_ref=sums_all.at[c],
            send_sem=send_c,
            recv_sem=recv_c,
            device_id=(t, peer, d),
            device_id_type=MESH,
        ).start()

    sums_all[c] = sums_here[...]
    others_c = pl.ds(0, num_cand - 1)
    pltpu.make_async_copy(sums_all.at[others_c], sums_all.at[others_c], recv_c).wait()
    both = sums_all[0]
    for s in range(1, num_cand):
        both = both + sums_all[s]
    loss[...] = jnp.log(both[0:1, :]) - both[1:2, :]
    loss_copy = pltpu.make_async_copy(loss, loss_out, out_sems.at[1])
    loss_copy.start()

    pltpu.make_async_copy(pooled.at[others], pooled.at[others], send_a).wait()
    pltpu.make_async_copy(gathered.at[others_b], gathered.at[others_b], send_b).wait()
    pltpu.make_async_copy(sums_all.at[others_c], sums_all.at[others_c], send_c).wait()
    emb_copy.wait()
    loss_copy.wait()


TILE = 256
EARLY = 2


def body(
    tables, bag_ids, bag_lengths, item_weight, user_features, user_w1, user_w2, positive_items
):
    sizes = tuple(lax.axis_size(n) for n in ("tab", "cand", "dp"))
    total = math.prod(sizes)
    slots = sizes[0] * sizes[2]
    table = tables[0]
    rows, width = table.shape
    items, length = bag_ids.shape[1:]
    per_block = items // total
    users = user_features.shape[0]
    embed = user_w2.shape[1]
    chunk = min(rows, 4096)
    chunks = rows // chunk
    held = min(chunks, 8)
    anywhere = pl.BlockSpec(memory_space=pl.ANY)
    item_emb, loss = pl.pallas_call(
        functools.partial(run_step, sizes),
        out_shape=(
            jax.ShapeDtypeStruct((per_block, embed), F32),
            jax.ShapeDtypeStruct((1, users), F32),
        ),
        in_specs=[anywhere] * 8,
        out_specs=(anywhere, anywhere),
        scratch_shapes=[
            pltpu.VMEM((length, items), jnp.int32),
            pltpu.VMEM((1, items), jnp.int32),
            pltpu.VMEM((length, items), jnp.int32),
            pltpu.VMEM((items, LANES), F32),
            pltpu.VMEM((held, chunk, width), BF16),
            pltpu.VMEM((rows + ZERO_ROWS, width), F32),
            pltpu.VMEM(item_weight.shape, BF16),
            pltpu.VMEM(user_features.shape, BF16),
            pltpu.VMEM(user_w1.shape, BF16),
            pltpu.VMEM(user_w2.shape, BF16),
            pltpu.VMEM((1, users), jnp.int32),
            pltpu.VMEM((total, per_block, width), F32),
            pltpu.VMEM((total, per_block, width), F32),
            pltpu.VMEM((per_block, item_weight.shape[0]), F32),
            pltpu.VMEM((per_block, embed), F32),
            pltpu.VMEM((users, embed), BF16),
            pltpu.VMEM((users, embed), BF16),
            pltpu.VMEM((slots, per_block, embed), F32),
            pltpu.VMEM((slots * per_block, embed), F32),
            pltpu.VMEM((2, users), F32),
            pltpu.VMEM((sizes[1], 2, users), F32),
            pltpu.VMEM((1, users), F32),
            pltpu.SemaphoreType.DMA((7,)),
            pltpu.SemaphoreType.DMA((chunks,)),
            pltpu.SemaphoreType.DMA((length,)),
            pltpu.SemaphoreType.DMA((2,)),
        ]
        + [pltpu.SemaphoreType.DMA] * 6
        + [pltpu.SemaphoreType.REGULAR]
        + [pltpu.SMEM((items,), jnp.int32)] * length,
        compiler_params=pltpu.CompilerParams(
            collective_id=0, has_side_effects=True, vmem_limit_bytes=VMEM_LIMIT
        ),
        name="step",
    )(
        bag_ids[0].T,
        bag_lengths,
        table,
        item_weight,
        user_features,
        user_w1,
        user_w2,
        positive_items[None, :],
    )
    return (item_emb, loss[0])


def solution(mesh):
    placed = (
        P(("cand", "dp"), "tab", None),
        P(("cand", "dp"), None, None),
        P(("cand", "dp"), None),
        P(),
        P(("tab", "dp"), None),
        P(),
        P(),
        P(("tab", "dp")),
    )
    return jax.shard_map(
        body,
        mesh=mesh,
        in_specs=placed,
        out_specs=(P(("tab", "cand", "dp"), None), P(("tab", "dp"))),
        check_vma=False,
    )
```

```python
import functools
import math

import jax
import jax.numpy as jnp
from jax import lax
from jax.experimental import pallas as pl
from jax.experimental.pallas import tpu as pltpu
from jax.sharding import PartitionSpec as P

epsilon = 1e-06
logit_scale = 20.0
MESH = pl.DeviceIdType.MESH
F32 = jnp.float32
BF16 = jnp.bfloat16
VMEM_LIMIT = 60 * 1024 * 1024
LANES = 128
SUBLANES = 8
ZERO_ROWS = 32


def split2(x):
    hi = x.astype(BF16)
    return hi, (x - hi.astype(F32)).astype(BF16)


def unit_rows(vectors):
    return vectors * lax.rsqrt(jnp.mean(vectors * vectors, axis=-1, keepdims=True) + epsilon)


def dot(a, b):
    return jnp.dot(a, b, preferred_element_type=F32)


def run_step(
    sizes,
    ids_in,
    lengths_in,
    table,
    weight_in,
    features_in,
    w1_in,
    w2_in,
    positives_in,
    emb_out,
    loss_out,
    ids_raw,
    lengths,
    index_rows,
    inverse,
    narrow,
    wide,
    weight,
    features,
    w1,
    w2,
    positives,
    pooled,
    arrived,
    joined,
    user_hi,
    user_lo,
    gathered,
    items_flat,
    sums_here,
    sums_all,
    load_sems,
    table_sems,
    index_sems,
    send_a,
    recv_a,
    send_b,
    recv_b,
    send_c,
    recv_c,
    ready,
    *index,
):
    num_tab, num_cand, num_dp = sizes
    total = num_tab * num_cand * num_dp
    groups = num_cand * num_dp
    slots = num_tab * num_dp
    t, c, d = (lax.axis_index(n) for n in ("tab", "cand", "dp"))
    me = (t * num_cand + c) * num_dp + d
    my_slot = t * num_dp + d
    per_block, width = pooled.shape[1:]
    items = total * per_block
    length = ids_raw.shape[0]
    rows, _ = table.shape
    users = features.shape[0]
    hidden = w1.shape[1]
    embed = w2.shape[1]
    chunks = table_sems.shape[0]
    chunk = rows // chunks
    held = narrow.shape[0]
    blocks_step = max(1, 32 // per_block)
    steps = total // blocks_step
    items_step = items // steps
    columns = items // LANES

    def place(index):
        return (index // groups, index // num_dp % num_cand, index % num_dp)

    barrier = pltpu.get_barrier_semaphore()

    loads = [
        pltpu.make_async_copy(a, b, load_sems.at[i])
        for i, (a, b) in enumerate(
            (
                (ids_in, ids_raw),
                (lengths_in, lengths),
                (w1_in, w1),
                (w2_in, w2),
                (features_in, features),
                (weight_in, weight),
                (positives_in, positives),
            )
        )
    ]

    def chunk_copy(n):
        part = pl.ds(pl.multiple_of(n * chunk, chunk), chunk)
        return pltpu.make_async_copy(table.at[part], narrow.at[lax.rem(n, held)], table_sems.at[n])

    def in_plane(slot):
        return (slot // num_dp, c, slot % num_dp)

    for load in loads[:2]:
        load.start()

    @pl.loop(1, num_cand)
    def _(j):
        peer = (t, lax.rem(c + j, num_cand), d)
        pl.semaphore_signal(barrier, inc=1, device_id=peer, device_id_type=MESH)

    @pl.loop(1, slots)
    def _(j):
        peer = in_plane(lax.rem(my_slot + j, slots))
        pl.semaphore_signal(barrier, inc=1, device_id=peer, device_id_type=MESH)

    for n in range(min(chunks, held)):
        chunk_copy(n).start()
    wide[pl.ds(rows, ZERO_ROWS), :] = jnp.zeros((ZERO_ROWS, width), F32)
    for load in loads[:2]:
        load.wait()
    first_row = t * rows
    spread = lax.broadcasted_iota(jnp.int32, (SUBLANES, LANES), 1) % 2 * (ZERO_ROWS // 2)
    line = lax.broadcasted_iota(jnp.int32, (SUBLANES, LANES), 0)
    for b in range(columns):
        lanes = slice(b * LANES, (b + 1) * LANES)
        count = lengths[:, lanes]
        for p in range(0, length, SUBLANES):
            local = ids_raw[p : p + SUBLANES, lanes] - first_row
            position = line + p
            keeping = (local >= 0) & (local < rows) & (position < count)
            spare = rows + position % (ZERO_ROWS // 2) + spread
            index_rows[p : p + SUBLANES, lanes] = jnp.where(keeping, local, spare)
    index_copies = [
        pltpu.make_async_copy(index_rows.at[p], index[p], index_sems.at[p]) for p in range(length)
    ]
    for copy in index_copies:
        copy.start()
    for b in range(columns):
        lanes = slice(b * LANES, (b + 1) * LANES)
        scale = 1.0 / lengths[:, lanes].astype(F32)
        inverse[lanes, :] = jnp.broadcast_to(scale, (LANES, LANES)).T

    pl.semaphore_wait(barrier, num_cand - 1 + slots - 1)

    @pl.loop(1, slots)
    def _(j):
        peer = in_plane(lax.rem(my_slot + j, slots))
        pl.semaphore_signal(ready, inc=1, device_id=peer, device_id_type=MESH)

    @pl.loop(0, chunks)
    def _(n):
        chunk_copy(n).wait()
        part = pl.ds(pl.multiple_of(n * chunk, chunk), chunk)
        wide[part, :] = narrow[lax.rem(n, held)].astype(F32)
        if held < chunks:

            @pl.when(n + held < chunks)
            def _():
                chunk_copy(n + held).start()

    for load in loads[2:]:
        load.start()
    for copy in index_copies:
        copy.wait()

    def send(dest):
        pltpu.make_async_remote_copy(
            src_ref=pooled.at[dest],
            dst_ref=arrived.at[me],
            send_sem=send_a,
            recv_sem=recv_a,
            device_id=place(dest),
            device_id_type=MESH,
        ).start()

    def group_at(s):
        if blocks_step > 1 or num_cand != 4:
            return lax.rem(me // blocks_step + 1 + s, steps)
        turn = s // slots
        plane = jnp.where(
            turn == 0,
            (c + 2) % 4,
            jnp.where(turn == 1, 3 - c, jnp.where(turn == 2, c + 1 - c % 2 * 2, c)),
        )
        slot = lax.rem(my_slot + 1 + s, slots)
        return (slot // num_dp * num_cand + plane) * num_dp + slot % num_dp

    @pl.loop(0, steps)
    def _(s):
        @pl.when(s == 1)
        def _():
            pl.semaphore_wait(ready, slots - 1)

        @pl.when(s > 0)
        def _():
            before = group_at(s - 1)
            for i in range(blocks_step):
                send(before * blocks_step + i)

        group = group_at(s)
        first = group * items_step
        for k in range(items_step):
            terms = [wide[pl.ds(of_place[first + k], 1), :] for of_place in index]
            while len(terms) > 1:
                terms = [a + b for a, b in zip(terms[::2], terms[1::2])] + (
                    [terms[-1]] if len(terms) % 2 else []
                )
            row = terms[0] * inverse[pl.ds(first + k, 1), :]
            pooled[group * blocks_step + k // per_block, pl.ds(k % per_block, 1), :] = row

    last = group_at(steps - 1)
    for i in range(blocks_step):
        dest = last * blocks_step + i
        if blocks_step > 1:

            @pl.when(dest != me)
            def _():
                send(dest)

    for load in loads[2:]:
        load.wait()
    tile = min(users, TILE)
    part_width = min(hidden, 256)

    def tower(n):
        user_rows = pl.ds(pl.multiple_of(n * tile, tile), tile)
        x = features[user_rows, :]
        pre = None
        for h in range(0, hidden, part_width):
            z = dot(x, w1[:, h : h + part_width])
            z = z * lax.erf(z * math.sqrt(0.5)) + z
            term = dot(z.astype(BF16), w2[h : h + part_width, :])
            pre = term if pre is None else pre + term
        hi, lo = split2(unit_rows(pre * 0.5) * (logit_scale / embed * math.log2(math.e)))
        user_hi[user_rows, :] = hi
        user_lo[user_rows, :] = lo

    tiles = users // tile
    early = tiles * EARLY // 8
    pl.loop(0, early)(tower)

    arrived[me] = pooled[me]
    others = pl.ds(0, total - 1)
    pltpu.make_async_copy(arrived.at[others], arrived.at[others], recv_a).wait()
    for f in range(groups):
        block = arrived[f]
        for s in range(1, num_tab):
            block = block + arrived[s * groups + f]
        joined[:, f * width : (f + 1) * width] = block
    hi, lo = split2(joined[...])
    both = dot(jnp.concatenate([hi, lo], axis=0), weight[...])
    item_emb = unit_rows(both[:per_block] + both[per_block:])
    emb_out[...] = item_emb

    @pl.loop(1, slots)
    def _(j):
        slot = lax.rem(my_slot + j, slots)
        pltpu.make_async_remote_copy(
            src_ref=emb_out,
            dst_ref=gathered.at[my_slot],
            send_sem=send_b,
            recv_sem=recv_b,
            device_id=in_plane(slot),
            device_id_type=MESH,
        ).start()

    gathered[my_slot] = item_emb
    pl.loop(early, tiles)(tower)
    others_b = pl.ds(0, slots - 1)
    pltpu.make_async_copy(gathered.at[others_b], gathered.at[others_b], recv_b).wait()
    for s in range(slots):
        items_flat[s * per_block : (s + 1) * per_block, :] = gathered[s]
    item_hi, item_lo = split2(items_flat[...])
    count = slots * per_block
    column = min(users, COLUMN)

    line = lax.broadcasted_iota(jnp.int32, (count, 1), 0)
    slot = line // per_block
    ids = ((slot // num_dp * num_cand + c) * num_dp + slot % num_dp) * per_block + line % per_block

    @pl.loop(0, users // column)
    def _(u):
        rows = pl.ds(pl.multiple_of(u * column, column), column)
        uh, ul = user_hi[rows, :], user_lo[rows, :]

        def cross(a, b):
            return lax.dot_general(a, b, (((1,), (1,)), ((), ())), preferred_element_type=F32)

        scores = cross(item_lo, uh) + cross(item_hi, ul) + cross(item_hi, uh)
        sums_here[0:1, rows] = jnp.sum(jnp.exp2(scores), axis=0, keepdims=True)
        sums_here[1:2, rows] = jnp.sum(
            jnp.where(ids == positives[:, rows], scores, jnp.float32(0.0)), axis=0, keepdims=True
        )

    @pl.loop(1, num_cand)
    def _(j):
        peer = lax.rem(c + j, num_cand)
        pltpu.make_async_remote_copy(
            src_ref=sums_here,
            dst_ref=sums_all.at[c],
            send_sem=send_c,
            recv_sem=recv_c,
            device_id=(t, peer, d),
            device_id_type=MESH,
        ).start()

    sums_all[c] = sums_here[...]
    others_c = pl.ds(0, num_cand - 1)
    pltpu.make_async_copy(sums_all.at[others_c], sums_all.at[others_c], recv_c).wait()
    both = sums_all[0]
    for s in range(1, num_cand):
        both = both + sums_all[s]
    loss_out[...] = jnp.log(both[0:1, :]) - both[1:2, :] * math.log(2.0)

    pltpu.make_async_copy(pooled.at[others], pooled.at[others], send_a).wait()
    pltpu.make_async_copy(gathered.at[others_b], gathered.at[others_b], send_b).wait()
    pltpu.make_async_copy(sums_all.at[others_c], sums_all.at[others_c], send_c).wait()


TILE = 512
EARLY = 2
COLUMN = 512


def body(
    tables, bag_ids, bag_lengths, item_weight, user_features, user_w1, user_w2, positive_items
):
    sizes = tuple(lax.axis_size(n) for n in ("tab", "cand", "dp"))
    total = math.prod(sizes)
    slots = sizes[0] * sizes[2]
    table = tables[0]
    rows, width = table.shape
    items, length = bag_ids.shape[1:]
    per_block = items // total
    users = user_features.shape[0]
    embed = user_w2.shape[1]
    chunk = min(rows, 4096)
    chunks = rows // chunk
    held = min(chunks, 8)
    far = pl.BlockSpec(memory_space=pltpu.HBM)
    near = pl.BlockSpec(memory_space=pltpu.VMEM)
    item_emb, loss = pl.pallas_call(
        functools.partial(run_step, sizes),
        out_shape=(
            pltpu.VMEM((per_block, embed), F32),
            pltpu.VMEM((1, users), F32),
        ),
        in_specs=[far] * 8,
        out_specs=(near, near),
        scratch_shapes=[
            pltpu.VMEM((length, items), jnp.int32),
            pltpu.VMEM((1, items), jnp.int32),
            pltpu.VMEM((length, items), jnp.int32),
            pltpu.VMEM((items, LANES), F32),
            pltpu.VMEM((held, chunk, width), BF16),
            pltpu.VMEM((rows + ZERO_ROWS, width), F32),
            pltpu.VMEM(item_weight.shape, BF16),
            pltpu.VMEM(user_features.shape, BF16),
            pltpu.VMEM(user_w1.shape, BF16),
            pltpu.VMEM(user_w2.shape, BF16),
            pltpu.VMEM((1, users), jnp.int32),
            pltpu.VMEM((total, per_block, width), F32),
            pltpu.VMEM((total, per_block, width), F32),
            pltpu.VMEM((per_block, item_weight.shape[0]), F32),
            pltpu.VMEM((users, embed), BF16),
            pltpu.VMEM((users, embed), BF16),
            pltpu.VMEM((slots, per_block, embed), F32),
            pltpu.VMEM((slots * per_block, embed), F32),
            pltpu.VMEM((2, users), F32),
            pltpu.VMEM((sizes[1], 2, users), F32),
            pltpu.SemaphoreType.DMA((7,)),
            pltpu.SemaphoreType.DMA((chunks,)),
            pltpu.SemaphoreType.DMA((length,)),
        ]
        + [pltpu.SemaphoreType.DMA] * 6
        + [pltpu.SemaphoreType.REGULAR]
        + [pltpu.SMEM((items,), jnp.int32)] * length,
        compiler_params=pltpu.CompilerParams(
            collective_id=0, has_side_effects=True, vmem_limit_bytes=VMEM_LIMIT
        ),
        name="step",
    )(
        bag_ids[0].T,
        bag_lengths,
        table,
        item_weight,
        user_features,
        user_w1,
        user_w2,
        positive_items[None, :],
    )
    return (item_emb, loss[0])


def solution(mesh):
    placed = (
        P(("cand", "dp"), "tab", None),
        P(("cand", "dp"), None, None),
        P(("cand", "dp"), None),
        P(),
        P(("tab", "dp"), None),
        P(),
        P(),
        P(("tab", "dp")),
    )
    return jax.shard_map(
        body,
        mesh=mesh,
        in_specs=placed,
        out_specs=(P(("tab", "cand", "dp"), None), P(("tab", "dp"))),
        check_vma=False,
    )
```

```python
import functools
import math

import jax
import jax.numpy as jnp
from jax import lax
from jax.experimental import pallas as pl
from jax.experimental.pallas import tpu as pltpu
from jax.sharding import PartitionSpec as P

epsilon = 1e-06
logit_scale = 20.0
MESH = pl.DeviceIdType.MESH
F32 = jnp.float32
BF16 = jnp.bfloat16
VMEM_LIMIT = 60 * 1024 * 1024
LANES = 128
SUBLANES = 8
ZERO_ROWS = 32


def split2(x):
    hi = x.astype(BF16)
    return hi, (x - hi.astype(F32)).astype(BF16)


def unit_rows(vectors):
    return vectors * lax.rsqrt(jnp.mean(vectors * vectors, axis=-1, keepdims=True) + epsilon)


def dot(a, b):
    return jnp.dot(a, b, preferred_element_type=F32)


def run_step(
    sizes,
    ids_in,
    lengths_in,
    table,
    weight_in,
    features_in,
    w1_in,
    w2_in,
    positives_in,
    emb_out,
    loss_out,
    ids_raw,
    lengths,
    index_rows,
    inverse,
    narrow,
    wide,
    weight,
    features,
    w1,
    w2,
    positives,
    pooled,
    arrived,
    helped,
    joined,
    user_hi,
    user_lo,
    gathered,
    items_flat,
    sums_here,
    sums_all,
    load_sems,
    table_sems,
    index_sems,
    send_a,
    recv_a,
    send_b,
    recv_b,
    send_c,
    recv_c,
    ready,
    recv_x,
    *index,
):
    num_tab, num_cand, num_dp = sizes
    total = num_tab * num_cand * num_dp
    groups = num_cand * num_dp
    slots = num_tab * num_dp
    t, c, d = (lax.axis_index(n) for n in ("tab", "cand", "dp"))
    me = (t * num_cand + c) * num_dp + d
    my_slot = t * num_dp + d
    per_block, width = pooled.shape[1:]
    items = total * per_block
    length = ids_raw.shape[0]
    rows, _ = table.shape
    users = features.shape[0]
    hidden = w1.shape[1]
    embed = w2.shape[1]
    chunks = table_sems.shape[0]
    chunk = rows // chunks
    held = narrow.shape[0]
    blocks_step = max(1, 32 // per_block)
    steps = total // blocks_step
    items_step = items // steps
    columns = items // LANES

    paired = num_tab == 2 and num_cand == 4 and num_dp % 2 == 0 and blocks_step == 1
    given_end = slots
    kept_start = slots + GAP
    kept_end = kept_start + slots
    far = lax.rem(c + lax.div(num_cand, 2), num_cand)
    mirror = num_cand - 1 - c
    near = c + 1 - 2 * lax.rem(c, 2)

    def place(index):
        return (
            lax.div(index, groups),
            lax.rem(lax.div(index, num_dp), num_cand),
            lax.rem(index, num_dp),
        )

    barrier = pltpu.get_barrier_semaphore()

    loads = [
        pltpu.make_async_copy(a, b, load_sems.at[i])
        for i, (a, b) in enumerate(
            (
                (ids_in, ids_raw),
                (lengths_in, lengths),
                (w1_in, w1),
                (w2_in, w2),
                (features_in, features),
                (weight_in, weight),
                (positives_in, positives),
            )
        )
    ]

    def chunk_copy(n):
        part = pl.ds(pl.multiple_of(n * chunk, chunk), chunk)
        return pltpu.make_async_copy(table.at[part], narrow.at[lax.rem(n, held)], table_sems.at[n])

    def in_plane(slot):
        return (lax.div(slot, num_dp), c, lax.rem(slot, num_dp))

    for load in loads[:2]:
        load.start()

    @pl.loop(1, num_cand)
    def _(j):
        peer = (t, lax.rem(c + j, num_cand), d)
        pl.semaphore_signal(barrier, inc=1, device_id=peer, device_id_type=MESH)

    for n in range(min(chunks, held)):
        chunk_copy(n).start()

    @pl.loop(1, slots)
    def _(j):
        peer = in_plane(lax.rem(my_slot + j, slots))
        pl.semaphore_signal(barrier, inc=1, device_id=peer, device_id_type=MESH)

    helped[slots] = jnp.zeros(helped.shape[1:], F32)
    wide[pl.ds(rows, ZERO_ROWS), :] = jnp.zeros((ZERO_ROWS, width), F32)
    for load in loads[:2]:
        load.wait()
    first_row = t * rows
    spread = lax.broadcasted_iota(jnp.int32, (SUBLANES, LANES), 1) % 2 * (ZERO_ROWS // 2)
    line = lax.broadcasted_iota(jnp.int32, (SUBLANES, LANES), 0)
    for b in range(columns):
        lanes = slice(b * LANES, (b + 1) * LANES)
        count = lengths[:, lanes]
        for p in range(0, length, SUBLANES):
            local = ids_raw[p : p + SUBLANES, lanes] - first_row
            position = line + p
            keeping = (local >= 0) & (local < rows) & (position < count)
            spare = rows + position % (ZERO_ROWS // 2) + spread
            index_rows[p : p + SUBLANES, lanes] = jnp.where(keeping, local, spare)
    index_copies = [
        pltpu.make_async_copy(index_rows.at[p], index[p], index_sems.at[p]) for p in range(length)
    ]
    for copy in index_copies:
        copy.start()
    for b in range(columns):
        lanes = slice(b * LANES, (b + 1) * LANES)
        scale = 1.0 / lengths[:, lanes].astype(F32)
        inverse[lanes, :] = jnp.broadcast_to(scale, (LANES, LANES)).T

    pl.semaphore_wait(barrier, num_cand - 1 + slots - 1)

    @pl.loop(1, slots)
    def _(j):
        peer = in_plane(lax.rem(my_slot + j, slots))
        pl.semaphore_signal(ready, inc=1, device_id=peer, device_id_type=MESH)

    @pl.loop(0, chunks)
    def _(n):
        chunk_copy(n).wait()
        part = pl.ds(pl.multiple_of(n * chunk, chunk), chunk)
        wide[part, :] = narrow[lax.rem(n, held)].astype(F32)
        if held < chunks:

            @pl.when(n + held < chunks)
            def _():
                chunk_copy(n + held).start()

    for load in loads[2:]:
        load.start()
    for copy in index_copies:
        copy.wait()

    def send(dest, slot):
        pltpu.make_async_remote_copy(
            src_ref=pooled.at[dest],
            dst_ref=arrived.at[slot],
            send_sem=send_a,
            recv_sem=recv_a,
            device_id=place(dest),
            device_id_type=MESH,
        ).start()

    def group_at(s):
        if not paired:
            return lax.rem(lax.div(me, blocks_step) + 1 + s, steps)
        i, j = turn_of(s)
        crossing = (s < given_end) | ((s >= kept_start) & (s < kept_end))
        k = lax.rem(j, slots)
        r = lax.rem(k, num_dp)
        pairs = num_dp // 2
        row = lax.rem(lax.div(d, 2) + pairs - 1 - lax.div(r, 2), pairs)
        close = row * 2 + lax.rem(d + 1 + r, 2)
        tab = jnp.where(
            crossing, jnp.where(s < given_end, 1 - t, t), jnp.where(k < num_dp, 1 - t, t)
        )
        dp = jnp.where(crossing, lax.rem(d + 1 + i, num_dp), close)
        plane = jnp.where(
            crossing,
            jnp.where(i < num_dp, far, mirror),
            jnp.where(j < slots, near, c),
        )
        return (tab * num_cand + plane) * num_dp + dp

    def turn_of(s):
        i = jnp.where(s < given_end, s, s - kept_start)
        j = s - jnp.where(s < kept_start, given_end, slots * 2)
        return i, j

    def send_group(s, group):
        if not paired:
            for i in range(blocks_step):
                send(group * blocks_step + i, me)
            return
        i, j = turn_of(s)

        @pl.when(s < given_end)
        def _():
            pltpu.make_async_remote_copy(
                src_ref=pooled.at[group],
                dst_ref=helped.at[i],
                send_sem=send_a,
                recv_sem=recv_x.at[i],
                device_id=(1 - t, c, d),
                device_id_type=MESH,
            ).start()

        @pl.when(s >= given_end)
        def _():
            kept = lax.div(i, num_dp) * num_dp + d
            direct = slots + jnp.where(j < slots, 0, slots) + my_slot
            send(group, jnp.where((s >= kept_start) & (s < kept_end), kept, direct))

    def gather(s, groups_then_now):
        before, groups_now = groups_then_now

        @pl.when(s == 1)
        def _():
            pl.semaphore_wait(ready, slots - 1)

        @pl.when(s > 0)
        def _():
            for i in range(AT_ONCE):
                send_group(s * AT_ONCE - AT_ONCE + i, before[i])

        if paired:

            @pl.when((s * AT_ONCE >= kept_start) & (s * AT_ONCE < kept_end))
            def _():
                for i in range(AT_ONCE):
                    block = helped.at[s * AT_ONCE + i - kept_start]
                    pltpu.make_async_copy(
                        block, block, recv_x.at[s * AT_ONCE + i - kept_start]
                    ).wait()

        for i in range(AT_ONCE):
            now = s * AT_ONCE + i
            group = groups_now[i]
            first = group * items_step
            if paired:
                keeps = (now >= kept_start) & (now < kept_end)
                help_at = jnp.where(keeps, now - kept_start, slots)
            for k in range(items_step):
                terms = [wide[pl.ds(of_place[first + k], 1), :] for of_place in index]
                while len(terms) > 1:
                    terms = [a + b for a, b in zip(terms[::2], terms[1::2])] + (
                        [terms[-1]] if len(terms) % 2 else []
                    )
                row = terms[0] * inverse[pl.ds(first + k, 1), :]
                if paired:
                    row = row + helped[help_at, pl.ds(k, 1), :]
                pooled[group * blocks_step + k // per_block, pl.ds(k % per_block, 1), :] = row

        return groups_now, groups_of(s + 1)

    def groups_of(s):
        return tuple(group_at(s * AT_ONCE + i) for i in range(AT_ONCE))

    start = groups_of(jnp.int32(0))
    finish, _ = lax.fori_loop(0, steps // AT_ONCE, gather, (start, start))
    for i in range(AT_ONCE - 1):
        send_group(jnp.int32(steps - AT_ONCE + i), finish[i])
    last = finish[AT_ONCE - 1]
    for i in range(blocks_step):
        dest = last * blocks_step + i
        if blocks_step > 1:

            @pl.when(dest != me)
            def _():
                send(dest, me)

    for load in loads[2:]:
        load.wait()
    tile = min(users, TILE)
    part_width = min(hidden, 256)

    def tower(n):
        user_rows = pl.ds(pl.multiple_of(n * tile, tile), tile)
        x = features[user_rows, :]
        pre = None
        for h in range(0, hidden, part_width):
            z = dot(x, w1[:, h : h + part_width])
            z = z * lax.erf(z * math.sqrt(0.5)) + z
            term = dot(z.astype(BF16), w2[h : h + part_width, :])
            pre = term if pre is None else pre + term
        hi, lo = split2(unit_rows(pre * 0.5) * (logit_scale / embed * math.log2(math.e)))
        user_hi[user_rows, :] = hi
        user_lo[user_rows, :] = lo

    tiles = users // tile
    early = tiles * EARLY // 8
    pl.loop(0, early)(tower)

    arrived[slots * 2 + my_slot if paired else me] = pooled[me]
    others = pl.ds(0, total - 1)
    landed = pl.ds(0, slots * 3 - 1 if paired else total - 1)
    pltpu.make_async_copy(arrived.at[landed], arrived.at[landed], recv_a).wait()

    def join(table, block):
        columns = pl.ds(pl.multiple_of(table * width, width), width)
        joined[:, columns] = block

    if paired:
        for f in range(num_dp):
            join(far * num_dp + f, arrived[f])
            join(mirror * num_dp + f, arrived[num_dp + f])
            for at, plane in ((slots, near), (slots * 2, c)):
                join(plane * num_dp + f, arrived[at + f] + arrived[at + num_dp + f])
    else:
        for f in range(groups):
            block = arrived[f]
            for s in range(1, num_tab):
                block = block + arrived[s * groups + f]
            join(f, block)
    hi, lo = split2(joined[...])
    both = dot(jnp.concatenate([hi, lo], axis=0), weight[...])
    item_emb = unit_rows(both[:per_block] + both[per_block:])
    emb_out[...] = item_emb

    @pl.loop(1, slots)
    def _(j):
        slot = lax.rem(my_slot + j, slots)
        pltpu.make_async_remote_copy(
            src_ref=emb_out,
            dst_ref=gathered.at[my_slot],
            send_sem=send_b,
            recv_sem=recv_b,
            device_id=in_plane(slot),
            device_id_type=MESH,
        ).start()

    gathered[my_slot] = item_emb
    pl.loop(early, tiles)(tower)
    others_b = pl.ds(0, slots - 1)
    pltpu.make_async_copy(gathered.at[others_b], gathered.at[others_b], recv_b).wait()
    for s in range(slots):
        items_flat[s * per_block : (s + 1) * per_block, :] = gathered[s]
    item_hi, item_lo = split2(items_flat[...])
    count = slots * per_block
    column = min(users, COLUMN)

    line = lax.broadcasted_iota(jnp.int32, (count, 1), 0)
    slot = line // per_block
    ids = ((slot // num_dp * num_cand + c) * num_dp + slot % num_dp) * per_block + line % per_block

    @pl.loop(0, users // column)
    def _(u):
        rows = pl.ds(pl.multiple_of(u * column, column), column)
        uh, ul = user_hi[rows, :], user_lo[rows, :]

        def cross(a, b):
            return lax.dot_general(a, b, (((1,), (1,)), ((), ())), preferred_element_type=F32)

        scores = cross(item_lo, uh) + cross(item_hi, ul) + cross(item_hi, uh)
        sums_here[0:1, rows] = jnp.sum(jnp.exp2(scores), axis=0, keepdims=True)
        sums_here[1:2, rows] = jnp.sum(
            jnp.where(ids == positives[:, rows], scores, jnp.float32(0.0)), axis=0, keepdims=True
        )

    for j in range(1, num_cand):
        peer = (mirror, far, near)[j - 1] if num_cand == 4 else lax.rem(c + j, num_cand)
        pltpu.make_async_remote_copy(
            src_ref=sums_here,
            dst_ref=sums_all.at[c],
            send_sem=send_c,
            recv_sem=recv_c,
            device_id=(t, peer, d),
            device_id_type=MESH,
        ).start()

    sums_all[c] = sums_here[...]
    others_c = pl.ds(0, num_cand - 1)
    pltpu.make_async_copy(sums_all.at[others_c], sums_all.at[others_c], recv_c).wait()
    both = sums_all[0]
    for s in range(1, num_cand):
        both = both + sums_all[s]
    loss_out[...] = jnp.log(both[0:1, :]) - both[1:2, :] * math.log(2.0)

    pltpu.make_async_copy(pooled.at[others], pooled.at[others], send_a).wait()
    pltpu.make_async_copy(gathered.at[others_b], gathered.at[others_b], send_b).wait()
    pltpu.make_async_copy(sums_all.at[others_c], sums_all.at[others_c], send_c).wait()


TILE = 512
EARLY = 2
AT_ONCE = 2
GAP = 2
COLUMN = 512


def body(
    tables, bag_ids, bag_lengths, item_weight, user_features, user_w1, user_w2, positive_items
):
    sizes = tuple(lax.axis_size(n) for n in ("tab", "cand", "dp"))
    total = math.prod(sizes)
    slots = sizes[0] * sizes[2]
    table = tables[0]
    rows, width = table.shape
    items, length = bag_ids.shape[1:]
    per_block = items // total
    users = user_features.shape[0]
    embed = user_w2.shape[1]
    chunk = min(rows, 4096)
    chunks = rows // chunk
    held = min(chunks, 8)
    far = pl.BlockSpec(memory_space=pltpu.HBM)
    near = pl.BlockSpec(memory_space=pltpu.VMEM)
    item_emb, loss = pl.pallas_call(
        functools.partial(run_step, sizes),
        out_shape=(
            pltpu.VMEM((per_block, embed), F32),
            pltpu.VMEM((1, users), F32),
        ),
        in_specs=[far] * 8,
        out_specs=(near, near),
        scratch_shapes=[
            pltpu.VMEM((length, items), jnp.int32),
            pltpu.VMEM((1, items), jnp.int32),
            pltpu.VMEM((length, items), jnp.int32),
            pltpu.VMEM((items, LANES), F32),
            pltpu.VMEM((held, chunk, width), BF16),
            pltpu.VMEM((rows + ZERO_ROWS, width), F32),
            pltpu.VMEM(item_weight.shape, BF16),
            pltpu.VMEM(user_features.shape, BF16),
            pltpu.VMEM(user_w1.shape, BF16),
            pltpu.VMEM(user_w2.shape, BF16),
            pltpu.VMEM((1, users), jnp.int32),
            pltpu.VMEM((total, per_block, width), F32),
            pltpu.VMEM((total, per_block, width), F32),
            pltpu.VMEM((slots + 1, per_block, width), F32),
            pltpu.VMEM((per_block, item_weight.shape[0]), F32),
            pltpu.VMEM((users, embed), BF16),
            pltpu.VMEM((users, embed), BF16),
            pltpu.VMEM((slots, per_block, embed), F32),
            pltpu.VMEM((slots * per_block, embed), F32),
            pltpu.VMEM((2, users), F32),
            pltpu.VMEM((sizes[1], 2, users), F32),
            pltpu.SemaphoreType.DMA((7,)),
            pltpu.SemaphoreType.DMA((chunks,)),
            pltpu.SemaphoreType.DMA((length,)),
        ]
        + [pltpu.SemaphoreType.DMA] * 6
        + [pltpu.SemaphoreType.REGULAR, pltpu.SemaphoreType.DMA((slots,))]
        + [pltpu.SMEM((items,), jnp.int32)] * length,
        compiler_params=pltpu.CompilerParams(
            collective_id=0, has_side_effects=True, vmem_limit_bytes=VMEM_LIMIT
        ),
        name="step",
    )(
        bag_ids[0].T,
        bag_lengths,
        table,
        item_weight,
        user_features,
        user_w1,
        user_w2,
        positive_items[None, :],
    )
    return (item_emb, loss[0])


def solution(mesh):
    placed = (
        P(("cand", "dp"), "tab", None),
        P(("cand", "dp"), None, None),
        P(("cand", "dp"), None),
        P(),
        P(("tab", "dp"), None),
        P(),
        P(),
        P(("tab", "dp")),
    )
    return jax.shard_map(
        body,
        mesh=mesh,
        in_specs=placed,
        out_specs=(P(("tab", "cand", "dp"), None), P(("tab", "dp"))),
        check_vma=False,
    )
```

```python
import functools
import math

import jax
import jax.numpy as jnp
from jax import lax
from jax.experimental import pallas as pl
from jax.experimental.pallas import tpu as pltpu
from jax.sharding import PartitionSpec as P

epsilon = 1e-06
logit_scale = 20.0
MESH = pl.DeviceIdType.MESH
F32 = jnp.float32
BF16 = jnp.bfloat16
VMEM_LIMIT = 60 * 1024 * 1024
LANES = 128
SUBLANES = 8
ZERO_ROWS = 32


def split2(x):
    hi = x.astype(BF16)
    return hi, (x - hi.astype(F32)).astype(BF16)


def unit_rows(vectors):
    return vectors * lax.rsqrt(jnp.mean(vectors * vectors, axis=-1, keepdims=True) + epsilon)


def dot(a, b):
    return jnp.dot(a, b, preferred_element_type=F32)


def run_step(
    sizes,
    ids_in,
    lengths_in,
    table,
    weight_in,
    features_in,
    w1_in,
    w2_in,
    positives_in,
    emb_out,
    loss_out,
    ids_raw,
    lengths,
    index_rows,
    inverse,
    narrow,
    wide,
    weight,
    features,
    w1,
    w2,
    positives,
    pooled,
    arrived,
    helped,
    joined,
    user_hi,
    user_lo,
    gathered,
    items_flat,
    sums_here,
    sums_all,
    load_sems,
    table_sems,
    index_sems,
    send_a,
    recv_a,
    send_b,
    recv_b,
    send_c,
    recv_c,
    ready,
    recv_x,
    *index,
):
    num_tab, num_cand, num_dp = sizes
    total = num_tab * num_cand * num_dp
    groups = num_cand * num_dp
    slots = num_tab * num_dp
    t, c, d = (lax.axis_index(n) for n in ("tab", "cand", "dp"))
    me = (t * num_cand + c) * num_dp + d
    my_slot = t * num_dp + d
    per_block, width = pooled.shape[1:]
    items = total * per_block
    length = ids_raw.shape[0]
    rows, _ = table.shape
    users = features.shape[0]
    hidden = w1.shape[1]
    embed = w2.shape[1]
    chunks = table_sems.shape[0]
    chunk = rows // chunks
    held = narrow.shape[0]
    blocks_step = max(1, 32 // per_block)
    steps = total // blocks_step
    items_step = items // steps
    columns = items // LANES

    paired = num_tab == 2 and num_cand == 4 and num_dp % 2 == 0 and blocks_step == 1
    given_end = slots
    kept_start = slots + GAP
    kept_end = kept_start + slots
    far = lax.rem(c + lax.div(num_cand, 2), num_cand)
    mirror = num_cand - 1 - c
    near = c + 1 - 2 * lax.rem(c, 2)

    def place(index):
        return (
            lax.div(index, groups),
            lax.rem(lax.div(index, num_dp), num_cand),
            lax.rem(index, num_dp),
        )

    barrier = pltpu.get_barrier_semaphore()

    loads = [
        pltpu.make_async_copy(a, b, load_sems.at[i])
        for i, (a, b) in enumerate(
            (
                (ids_in, ids_raw),
                (lengths_in, lengths),
                (w1_in, w1),
                (w2_in, w2),
                (features_in, features),
                (weight_in, weight),
                (positives_in, positives),
            )
        )
    ]

    def chunk_copy(n):
        part = pl.ds(pl.multiple_of(n * chunk, chunk), chunk)
        return pltpu.make_async_copy(table.at[part], narrow.at[lax.rem(n, held)], table_sems.at[n])

    def in_plane(slot):
        return (lax.div(slot, num_dp), c, lax.rem(slot, num_dp))

    for load in loads[:2]:
        load.start()

    @pl.loop(1, num_cand)
    def _(j):
        peer = (t, lax.rem(c + j, num_cand), d)
        pl.semaphore_signal(barrier, inc=1, device_id=peer, device_id_type=MESH)

    for n in range(min(chunks, held)):
        chunk_copy(n).start()

    @pl.loop(1, slots)
    def _(j):
        peer = in_plane(lax.rem(my_slot + j, slots))
        pl.semaphore_signal(barrier, inc=1, device_id=peer, device_id_type=MESH)

    helped[slots] = jnp.zeros(helped.shape[1:], F32)
    wide[pl.ds(rows, ZERO_ROWS), :] = jnp.zeros((ZERO_ROWS, width), F32)
    for load in loads[:2]:
        load.wait()
    first_row = t * rows
    spread = lax.broadcasted_iota(jnp.int32, (SUBLANES, LANES), 1) % 2 * (ZERO_ROWS // 2)
    line = lax.broadcasted_iota(jnp.int32, (SUBLANES, LANES), 0)
    for b in range(columns):
        lanes = slice(b * LANES, (b + 1) * LANES)
        count = lengths[:, lanes]
        for p in range(0, length, SUBLANES):
            local = ids_raw[p : p + SUBLANES, lanes] - first_row
            position = line + p
            keeping = (local >= 0) & (local < rows) & (position < count)
            spare = rows + position % (ZERO_ROWS // 2) + spread
            index_rows[p : p + SUBLANES, lanes] = jnp.where(keeping, local, spare)
    index_copies = [
        pltpu.make_async_copy(index_rows.at[p], index[p], index_sems.at[p]) for p in range(length)
    ]
    for copy in index_copies:
        copy.start()
    for b in range(columns):
        lanes = slice(b * LANES, (b + 1) * LANES)
        scale = 1.0 / lengths[:, lanes].astype(F32)
        inverse[lanes, :] = jnp.broadcast_to(scale, (LANES, LANES)).T

    pl.semaphore_wait(barrier, num_cand - 1 + slots - 1)

    @pl.loop(1, slots)
    def _(j):
        peer = in_plane(lax.rem(my_slot + j, slots))
        pl.semaphore_signal(ready, inc=1, device_id=peer, device_id_type=MESH)

    @pl.loop(0, chunks)
    def _(n):
        chunk_copy(n).wait()
        part = pl.ds(pl.multiple_of(n * chunk, chunk), chunk)
        wide[part, :] = narrow[lax.rem(n, held)].astype(F32)
        if held < chunks:

            @pl.when(n + held < chunks)
            def _():
                chunk_copy(n + held).start()

    for load in loads[2:]:
        load.start()
    for copy in index_copies:
        copy.wait()

    def send(dest, slot):
        pltpu.make_async_remote_copy(
            src_ref=pooled.at[dest],
            dst_ref=arrived.at[slot],
            send_sem=send_a,
            recv_sem=recv_a,
            device_id=place(dest),
            device_id_type=MESH,
        ).start()

    def plane_slot(k):
        r = lax.rem(k, num_dp)
        pairs = num_dp // 2
        row = lax.rem(lax.div(d, 2) + pairs - 1 - lax.div(r, 2), pairs)
        tab = jnp.where(k < num_dp, 1 - t, t)
        return tab * num_dp + row * 2 + lax.rem(d + 1 + r, 2)

    def group_at(s):
        if not paired:
            return lax.rem(lax.div(me, blocks_step) + 1 + s, steps)
        i, j = turn_of(s)
        crossing = (s < given_end) | ((s >= kept_start) & (s < kept_end))
        k = lax.rem(j, slots)
        close = plane_slot(k)
        tab = jnp.where(
            crossing, jnp.where(s < given_end, 1 - t, t), lax.div(close, num_dp)
        )
        dp = lax.rem(jnp.where(crossing, d + 1 + i, close), num_dp)
        plane = jnp.where(
            crossing,
            jnp.where(i < num_dp, far, mirror),
            jnp.where(j < slots, near, c),
        )
        return (tab * num_cand + plane) * num_dp + dp

    def turn_of(s):
        i = jnp.where(s < given_end, s, s - kept_start)
        j = s - jnp.where(s < kept_start, given_end, slots * 2)
        return i, j

    def send_group(s, group):
        if not paired:
            for i in range(blocks_step):
                send(group * blocks_step + i, me)
            return
        i, j = turn_of(s)

        @pl.when(s < given_end)
        def _():
            pltpu.make_async_remote_copy(
                src_ref=pooled.at[group],
                dst_ref=helped.at[i],
                send_sem=send_a,
                recv_sem=recv_x.at[i],
                device_id=(1 - t, c, d),
                device_id_type=MESH,
            ).start()

        @pl.when(s >= given_end)
        def _():
            kept = lax.div(i, num_dp) * num_dp + d
            direct = slots + jnp.where(j < slots, 0, slots) + my_slot
            send(group, jnp.where((s >= kept_start) & (s < kept_end), kept, direct))

    def gather(s, groups_then_now):
        before, groups_now = groups_then_now

        @pl.when(s == 1)
        def _():
            pl.semaphore_wait(ready, slots - 1)

        @pl.when(s > 0)
        def _():
            for i in range(AT_ONCE):
                send_group(s * AT_ONCE - AT_ONCE + i, before[i])

        if paired:

            @pl.when((s * AT_ONCE >= kept_start) & (s * AT_ONCE < kept_end))
            def _():
                for i in range(AT_ONCE):
                    block = helped.at[s * AT_ONCE + i - kept_start]
                    pltpu.make_async_copy(
                        block, block, recv_x.at[s * AT_ONCE + i - kept_start]
                    ).wait()

        for i in range(AT_ONCE):
            now = s * AT_ONCE + i
            group = groups_now[i]
            first = group * items_step
            if paired:
                keeps = (now >= kept_start) & (now < kept_end)
                help_at = jnp.where(keeps, now - kept_start, slots)
            for k in range(items_step):
                terms = [wide[pl.ds(of_place[first + k], 1), :] for of_place in index]
                while len(terms) > 1:
                    terms = [a + b for a, b in zip(terms[::2], terms[1::2])] + (
                        [terms[-1]] if len(terms) % 2 else []
                    )
                row = terms[0] * inverse[pl.ds(first + k, 1), :]
                if paired:
                    row = row + helped[help_at, pl.ds(k, 1), :]
                pooled[group * blocks_step + k // per_block, pl.ds(k % per_block, 1), :] = row

        return groups_now, groups_of(s + 1)

    def groups_of(s):
        return tuple(group_at(s * AT_ONCE + i) for i in range(AT_ONCE))

    start = groups_of(jnp.int32(0))
    finish, _ = lax.fori_loop(0, steps // AT_ONCE, gather, (start, start))
    for i in range(AT_ONCE - 1):
        send_group(jnp.int32(steps - AT_ONCE + i), finish[i])
    last = finish[AT_ONCE - 1]
    for i in range(blocks_step):
        dest = last * blocks_step + i
        if blocks_step > 1:

            @pl.when(dest != me)
            def _():
                send(dest, me)

    for load in loads[2:]:
        load.wait()
    tile = min(users, TILE)
    part_width = min(hidden, 256)

    def tower(n):
        user_rows = pl.ds(pl.multiple_of(n * tile, tile), tile)
        x = features[user_rows, :]
        pre = None
        for h in range(0, hidden, part_width):
            z = dot(x, w1[:, h : h + part_width])
            z = z * lax.erf(z * math.sqrt(0.5)) + z
            term = dot(z.astype(BF16), w2[h : h + part_width, :])
            pre = term if pre is None else pre + term
        hi, lo = split2(unit_rows(pre * 0.5) * (logit_scale / embed * math.log2(math.e)))
        user_hi[user_rows, :] = hi
        user_lo[user_rows, :] = lo

    tiles = users // tile
    early = tiles * EARLY // 8
    pl.loop(0, early)(tower)

    arrived[slots * 2 + my_slot if paired else me] = pooled[me]
    others = pl.ds(0, total - 1)
    landed = pl.ds(0, slots * 3 - 1 if paired else total - 1)
    pltpu.make_async_copy(arrived.at[landed], arrived.at[landed], recv_a).wait()

    def join(table, block):
        columns = pl.ds(pl.multiple_of(table * width, width), width)
        joined[:, columns] = block

    if paired:
        for f in range(num_dp):
            join(far * num_dp + f, arrived[f])
            join(mirror * num_dp + f, arrived[num_dp + f])
            for at, plane in ((slots, near), (slots * 2, c)):
                join(plane * num_dp + f, arrived[at + f] + arrived[at + num_dp + f])
    else:
        for f in range(groups):
            block = arrived[f]
            for s in range(1, num_tab):
                block = block + arrived[s * groups + f]
            join(f, block)
    hi, lo = split2(joined[...])
    both = dot(jnp.concatenate([hi, lo], axis=0), weight[...])
    item_emb = unit_rows(both[:per_block] + both[per_block:])
    emb_out[...] = item_emb

    @pl.loop(0, slots - 1)
    def _(k):
        slot = plane_slot(k) if paired else lax.rem(my_slot + 1 + k, slots)
        pltpu.make_async_remote_copy(
            src_ref=emb_out,
            dst_ref=gathered.at[my_slot],
            send_sem=send_b,
            recv_sem=recv_b,
            device_id=in_plane(slot),
            device_id_type=MESH,
        ).start()

    gathered[my_slot] = item_emb
    pl.loop(early, tiles)(tower)
    others_b = pl.ds(0, slots - 1)
    pltpu.make_async_copy(gathered.at[others_b], gathered.at[others_b], recv_b).wait()
    for s in range(slots):
        items_flat[s * per_block : (s + 1) * per_block, :] = gathered[s]
    item_hi, item_lo = split2(items_flat[...])
    count = slots * per_block
    column = min(users, COLUMN)

    line = lax.broadcasted_iota(jnp.int32, (count, 1), 0)
    slot = line // per_block
    ids = ((slot // num_dp * num_cand + c) * num_dp + slot % num_dp) * per_block + line % per_block

    @pl.loop(0, users // column)
    def _(u):
        rows = pl.ds(pl.multiple_of(u * column, column), column)
        uh, ul = user_hi[rows, :], user_lo[rows, :]

        def cross(a, b):
            return lax.dot_general(a, b, (((1,), (1,)), ((), ())), preferred_element_type=F32)

        scores = cross(item_lo, uh) + cross(item_hi, ul) + cross(item_hi, uh)
        sums_here[0:1, rows] = jnp.sum(jnp.exp2(scores), axis=0, keepdims=True)
        sums_here[1:2, rows] = jnp.sum(
            jnp.where(ids == positives[:, rows], scores, jnp.float32(0.0)), axis=0, keepdims=True
        )

    for j in range(1, num_cand):
        peer = (mirror, far, near)[j - 1] if num_cand == 4 else lax.rem(c + j, num_cand)
        pltpu.make_async_remote_copy(
            src_ref=sums_here,
            dst_ref=sums_all.at[c],
            send_sem=send_c,
            recv_sem=recv_c,
            device_id=(t, peer, d),
            device_id_type=MESH,
        ).start()

    sums_all[c] = sums_here[...]
    others_c = pl.ds(0, num_cand - 1)
    pltpu.make_async_copy(sums_all.at[others_c], sums_all.at[others_c], recv_c).wait()
    both = sums_all[0]
    for s in range(1, num_cand):
        both = both + sums_all[s]
    loss_out[...] = jnp.log(both[0:1, :]) - both[1:2, :] * math.log(2.0)

    pltpu.make_async_copy(pooled.at[others], pooled.at[others], send_a).wait()
    pltpu.make_async_copy(gathered.at[others_b], gathered.at[others_b], send_b).wait()
    pltpu.make_async_copy(sums_all.at[others_c], sums_all.at[others_c], send_c).wait()


TILE = 512
EARLY = 2
AT_ONCE = 2
GAP = 2
COLUMN = 2048


def keep(emb_in, loss_in, emb_out, loss_out, sems):
    pairs = ((emb_in, emb_out), (loss_in, loss_out))
    copies = [pltpu.make_async_copy(a, b, sems.at[i]) for i, (a, b) in enumerate(pairs)]
    for copy in copies:
        copy.start()
    for copy in copies:
        copy.wait()


def body(
    tables, bag_ids, bag_lengths, item_weight, user_features, user_w1, user_w2, positive_items
):
    sizes = tuple(lax.axis_size(n) for n in ("tab", "cand", "dp"))
    total = math.prod(sizes)
    slots = sizes[0] * sizes[2]
    table = tables[0]
    rows, width = table.shape
    items, length = bag_ids.shape[1:]
    per_block = items // total
    users = user_features.shape[0]
    embed = user_w2.shape[1]
    chunk = min(rows, 4096)
    chunks = rows // chunk
    held = min(chunks, 8)
    anywhere = pl.BlockSpec(memory_space=pl.ANY)
    near = pl.BlockSpec(memory_space=pltpu.VMEM)
    item_emb, loss = pl.pallas_call(
        functools.partial(run_step, sizes),
        out_shape=(
            pltpu.VMEM((per_block, embed), F32),
            pltpu.VMEM((1, users), F32),
        ),
        in_specs=[anywhere] * 8,
        out_specs=(near, near),
        scratch_shapes=[
            pltpu.VMEM((length, items), jnp.int32),
            pltpu.VMEM((1, items), jnp.int32),
            pltpu.VMEM((length, items), jnp.int32),
            pltpu.VMEM((items, LANES), F32),
            pltpu.VMEM((held, chunk, width), BF16),
            pltpu.VMEM((rows + ZERO_ROWS, width), F32),
            pltpu.VMEM(item_weight.shape, BF16),
            pltpu.VMEM(user_features.shape, BF16),
            pltpu.VMEM(user_w1.shape, BF16),
            pltpu.VMEM(user_w2.shape, BF16),
            pltpu.VMEM((1, users), jnp.int32),
            pltpu.VMEM((total, per_block, width), F32),
            pltpu.VMEM((total, per_block, width), F32),
            pltpu.VMEM((slots + 1, per_block, width), F32),
            pltpu.VMEM((per_block, item_weight.shape[0]), F32),
            pltpu.VMEM((users, embed), BF16),
            pltpu.VMEM((users, embed), BF16),
            pltpu.VMEM((slots, per_block, embed), F32),
            pltpu.VMEM((slots * per_block, embed), F32),
            pltpu.VMEM((2, users), F32),
            pltpu.VMEM((sizes[1], 2, users), F32),
            pltpu.SemaphoreType.DMA((7,)),
            pltpu.SemaphoreType.DMA((chunks,)),
            pltpu.SemaphoreType.DMA((length,)),
        ]
        + [pltpu.SemaphoreType.DMA] * 6
        + [pltpu.SemaphoreType.REGULAR, pltpu.SemaphoreType.DMA((slots,))]
        + [pltpu.SMEM((items,), jnp.int32)] * length,
        compiler_params=pltpu.CompilerParams(
            collective_id=0, has_side_effects=True, vmem_limit_bytes=VMEM_LIMIT
        ),
        name="step",
    )(
        bag_ids[0].T,
        bag_lengths,
        table,
        item_weight,
        user_features,
        user_w1,
        user_w2,
        positive_items[None, :],
    )
    item_emb, loss = pl.pallas_call(
        keep,
        out_shape=(
            jax.ShapeDtypeStruct((per_block, embed), F32),
            jax.ShapeDtypeStruct((1, users), F32),
        ),
        in_specs=[pl.BlockSpec(memory_space=pltpu.VMEM)] * 2,
        out_specs=(anywhere, anywhere),
        scratch_shapes=[pltpu.SemaphoreType.DMA((2,))],
        name="keep",
    )(*[pltpu.with_memory_space_constraint(x, pltpu.VMEM) for x in (item_emb, loss)])
    return (item_emb, loss[0])


def solution(mesh):
    placed = (
        P(("cand", "dp"), "tab", None),
        P(("cand", "dp"), None, None),
        P(("cand", "dp"), None),
        P(),
        P(("tab", "dp"), None),
        P(),
        P(),
        P(("tab", "dp")),
    )
    return jax.shard_map(
        body,
        mesh=mesh,
        in_specs=placed,
        out_specs=(P(("tab", "cand", "dp"), None), P(("tab", "dp"))),
        check_vma=False,
    )
```

```python
import functools
import math

import jax
import jax.numpy as jnp
from jax import lax
from jax.experimental import pallas as pl
from jax.experimental.pallas import tpu as pltpu
from jax.sharding import PartitionSpec as P

epsilon = 1e-06
logit_scale = 20.0
MESH = pl.DeviceIdType.MESH
F32 = jnp.float32
BF16 = jnp.bfloat16
VMEM_LIMIT = 60 * 1024 * 1024
LANES = 128
SUBLANES = 8
ZERO_ROWS = 32


def split2(x):
    hi = x.astype(BF16)
    return hi, (x - hi.astype(F32)).astype(BF16)


def unit_rows(vectors):
    return vectors * lax.rsqrt(jnp.mean(vectors * vectors, axis=-1, keepdims=True) + epsilon)


def dot(a, b):
    return jnp.dot(a, b, preferred_element_type=F32)


def run_step(
    sizes,
    ids_in,
    lengths_in,
    table,
    weight_in,
    features_in,
    w1_in,
    w2_in,
    positives_in,
    emb_out,
    loss_out,
    ids_raw,
    lengths,
    index_rows,
    inverse,
    narrow,
    wide,
    weight,
    features,
    w1,
    w2,
    positives,
    pooled,
    arrived,
    helped,
    user_hi,
    user_lo,
    gathered,
    items_flat,
    sums_here,
    sums_all,
    load_sems,
    table_sems,
    index_sems,
    send_a,
    recv_a,
    send_b,
    recv_b,
    send_c,
    recv_c,
    ready,
    recv_x,
    *index,
):
    num_tab, num_cand, num_dp = sizes
    total = num_tab * num_cand * num_dp
    groups = num_cand * num_dp
    slots = num_tab * num_dp
    t, c, d = (lax.axis_index(n) for n in ("tab", "cand", "dp"))
    me = (t * num_cand + c) * num_dp + d
    my_slot = t * num_dp + d
    per_block, width = pooled.shape[1:]
    items = total * per_block
    length = ids_raw.shape[0]
    rows, _ = table.shape
    users = features.shape[0]
    hidden = w1.shape[1]
    embed = w2.shape[1]
    chunks = table_sems.shape[0]
    chunk = rows // chunks
    held = narrow.shape[0]
    blocks_step = max(1, 32 // per_block)
    steps = total // blocks_step
    items_step = items // steps
    columns = items // LANES

    paired = num_tab == 2 and num_cand == 4 and num_dp == 4 and blocks_step == 1
    given_end = slots
    kept_start = slots + GAP
    kept_end = kept_start + slots
    far = lax.rem(c + lax.div(num_cand, 2), num_cand)
    mirror = num_cand - 1 - c
    near = c + 1 - 2 * lax.rem(c, 2)

    def place(index):
        return (
            lax.div(index, groups),
            lax.rem(lax.div(index, num_dp), num_cand),
            lax.rem(index, num_dp),
        )

    barrier = pltpu.get_barrier_semaphore()

    loads = [
        pltpu.make_async_copy(a, b, load_sems.at[i])
        for i, (a, b) in enumerate(
            (
                (ids_in, ids_raw),
                (lengths_in, lengths),
                (w1_in, w1),
                (w2_in, w2),
                (features_in, features),
                (weight_in, weight),
                (positives_in, positives),
            )
        )
    ]

    def chunk_copy(n):
        part = pl.ds(pl.multiple_of(n * chunk, chunk), chunk)
        return pltpu.make_async_copy(table.at[part], narrow.at[lax.rem(n, held)], table_sems.at[n])

    def in_plane(slot):
        return (lax.div(slot, num_dp), c, lax.rem(slot, num_dp))

    for load in loads[:2]:
        load.start()

    @pl.loop(1, num_cand)
    def _(j):
        peer = (t, lax.rem(c + j, num_cand), d)
        pl.semaphore_signal(barrier, inc=1, device_id=peer, device_id_type=MESH)

    for n in range(min(chunks, held)):
        chunk_copy(n).start()

    @pl.loop(1, slots)
    def _(j):
        peer = in_plane(lax.rem(my_slot + j, slots))
        pl.semaphore_signal(barrier, inc=1, device_id=peer, device_id_type=MESH)

    helped[slots] = jnp.zeros(helped.shape[1:], F32)
    wide[pl.ds(rows, ZERO_ROWS), :] = jnp.zeros((ZERO_ROWS, width), F32)
    for load in loads[:2]:
        load.wait()
    first_row = t * rows
    spread = lax.broadcasted_iota(jnp.int32, (SUBLANES, LANES), 1) % 2 * (ZERO_ROWS // 2)
    line = lax.broadcasted_iota(jnp.int32, (SUBLANES, LANES), 0)
    for b in range(columns):
        lanes = slice(b * LANES, (b + 1) * LANES)
        count = lengths[:, lanes]
        for p in range(0, length, SUBLANES):
            local = ids_raw[p : p + SUBLANES, lanes] - first_row
            position = line + p
            keeping = (local >= 0) & (local < rows) & (position < count)
            spare = rows + position % (ZERO_ROWS // 2) + spread
            index_rows[p : p + SUBLANES, lanes] = jnp.where(keeping, local, spare)
    index_copies = [
        pltpu.make_async_copy(index_rows.at[p], index[p], index_sems.at[p]) for p in range(length)
    ]
    for copy in index_copies:
        copy.start()
    for b in range(columns):
        lanes = slice(b * LANES, (b + 1) * LANES)
        scale = 1.0 / lengths[:, lanes].astype(F32)
        inverse[lanes, :] = jnp.broadcast_to(scale, (LANES, LANES)).T

    pl.semaphore_wait(barrier, num_cand - 1 + slots - 1)

    @pl.loop(1, slots)
    def _(j):
        peer = in_plane(lax.rem(my_slot + j, slots))
        pl.semaphore_signal(ready, inc=1, device_id=peer, device_id_type=MESH)

    @pl.loop(0, chunks)
    def _(n):
        chunk_copy(n).wait()
        part = pl.ds(pl.multiple_of(n * chunk, chunk), chunk)
        wide[part, :] = narrow[lax.rem(n, held)].astype(F32)
        if held < chunks:

            @pl.when(n + held < chunks)
            def _():
                chunk_copy(n + held).start()

    for load in loads[2:]:
        load.start()
    for copy in index_copies:
        copy.wait()

    def send(dest, slot):
        pltpu.make_async_remote_copy(
            src_ref=pooled.at[dest],
            dst_ref=arrived.at[slot],
            send_sem=send_a,
            recv_sem=recv_a.at[0],
            device_id=place(dest),
            device_id_type=MESH,
        ).start()

    def plane_slot(k):
        outer = k < num_tab
        inner = k >= num_tab + num_dp
        even = lax.rem(k, 2) == 0
        over_tab = outer | (even & ~inner)
        over_row = outer | (~even & ~inner)
        shift = jnp.where(outer | inner, k + 1, lax.div(k, 2))
        tab = jnp.where(over_tab, 1 - t, t)
        row = lax.div(d, 2)
        row = jnp.where(over_row, 1 - row, row)
        return tab * num_dp + row * 2 + lax.rem(d + shift, 2)

    def block_at(s):
        if not paired:
            group = lax.rem(lax.div(me, blocks_step) + 1 + s, steps)
            return (group,)
        i = jnp.where(s < given_end, s, s - kept_start)
        j = s - jnp.where(s < kept_start, given_end, slots * 2)
        close = plane_slot(lax.rem(j, slots))
        crossing = (s < given_end) | ((s >= kept_start) & (s < kept_end))
        tab = jnp.where(
            crossing, jnp.where(s < given_end, 1 - t, t), lax.div(close, num_dp)
        )
        dp = lax.rem(jnp.where(crossing, d + 1 + i, close), num_dp)
        plane = jnp.where(
            crossing,
            jnp.where(i < num_dp, far, mirror),
            jnp.where(j < slots, near, c),
        )
        kept = jnp.where(i < num_dp, 0, num_dp) + d
        direct = jnp.where(j < slots, slots, slots * 2) + my_slot
        target = jnp.where(crossing, jnp.where(s < given_end, i, kept), direct)
        return ((tab * num_cand + plane) * num_dp + dp, tab, plane, dp, target)

    def send_block(s, block, given):
        if not paired:
            for i in range(blocks_step):
                send(block[0] * blocks_step + i, me)
            return
        group, tab, plane, dp, target = block
        if given:
            arrival = helped.at[target], recv_x.at[target], (1 - t, c, d)
        else:
            keeps = (s >= kept_start) & (s < kept_end)
            arrival = arrived.at[target], recv_a.at[jnp.where(keeps, 1, 0)], (tab, plane, dp)
        pltpu.make_async_remote_copy(
            src_ref=pooled.at[group],
            dst_ref=arrival[0],
            send_sem=send_a,
            recv_sem=arrival[1],
            device_id=arrival[2],
            device_id_type=MESH,
        ).start()

    def gather(s, groups_then_now):
        before, groups_now = groups_then_now

        def sends(given):
            for i in range(AT_ONCE):
                send_block(s * AT_ONCE - AT_ONCE + i, before[i], given)

        if paired:

            @pl.when((s > 0) & (s * AT_ONCE <= given_end))
            def _():
                @pl.when(s == 1)
                def _():
                    pl.semaphore_wait(ready, slots - 1)

                sends(True)

            @pl.when(s * AT_ONCE > given_end)
            def _():
                sends(False)

            @pl.when((s * AT_ONCE >= kept_start) & (s * AT_ONCE < kept_end))
            def _():
                for i in range(AT_ONCE):
                    at = s * AT_ONCE + i - kept_start
                    block = helped.at[at]
                    pltpu.make_async_copy(block, block, recv_x.at[at]).wait()
        else:

            @pl.when(s > 0)
            def _():
                @pl.when(s == 1)
                def _():
                    pl.semaphore_wait(ready, slots - 1)

                sends(False)

        for i in range(AT_ONCE):
            now = s * AT_ONCE + i
            group = groups_now[i][0]
            first = group * items_step
            if paired:
                keeps = (now >= kept_start) & (now < kept_end)
                help_at = jnp.where(keeps, now - kept_start, slots)
            for k in range(items_step):
                terms = [wide[pl.ds(of_place[first + k], 1), :] for of_place in index]
                while len(terms) > 1:
                    terms = [a + b for a, b in zip(terms[::2], terms[1::2])] + (
                        [terms[-1]] if len(terms) % 2 else []
                    )
                row = terms[0] * inverse[pl.ds(first + k, 1), :]
                if paired:
                    row = row + helped[help_at, pl.ds(k, 1), :]
                pooled[group * blocks_step + k // per_block, pl.ds(k % per_block, 1), :] = row

        return groups_now, groups_of(s + 1)

    def groups_of(s):
        return tuple(block_at(s * AT_ONCE + i) for i in range(AT_ONCE))

    start = groups_of(jnp.int32(0))
    finish, _ = lax.fori_loop(0, steps // AT_ONCE, gather, (start, start))
    for i in range(AT_ONCE - 1):
        send_block(jnp.int32(steps - AT_ONCE + i), finish[i], False)
    last = finish[AT_ONCE - 1][0]
    for i in range(blocks_step):
        dest = last * blocks_step + i
        if blocks_step > 1:

            @pl.when(dest != me)
            def _():
                send(dest, me)

    for load in loads[2:]:
        load.wait()
    tile = min(users, TILE)
    part_width = min(hidden, 256)

    def tower(n):
        user_rows = pl.ds(pl.multiple_of(n * tile, tile), tile)
        x = features[user_rows, :]
        pre = None
        for h in range(0, hidden, part_width):
            z = dot(x, w1[:, h : h + part_width])
            z = z * lax.erf(z * math.sqrt(0.5)) + z
            term = dot(z.astype(BF16), w2[h : h + part_width, :])
            pre = term if pre is None else pre + term
        hi, lo = split2(unit_rows(pre * 0.5) * (logit_scale / embed * math.log2(math.e)))
        user_hi[user_rows, :] = hi
        user_lo[user_rows, :] = lo

    tiles = users // tile
    early = tiles * EARLY // 8
    pl.loop(0, early)(tower)

    others = pl.ds(0, total - 1)

    def wait_blocks(first, number, kind):
        blocks = arrived.at[pl.ds(first, number)]
        pltpu.make_async_copy(blocks, blocks, recv_a.at[kind]).wait()

    def project(planes):
        depth = num_dp * width
        result = None
        for plane, blocks in planes:
            part = jnp.concatenate(split2(jnp.concatenate(blocks, axis=1)), axis=0)
            at = pl.ds(pl.multiple_of(plane * depth, depth), depth)
            term = dot(part, weight[at, :])
            result = term if result is None else result + term
        return result[:per_block] + result[per_block:]

    if paired:
        wait_blocks(0, slots, 1)
        crossed = project(
            (plane, [arrived[at + f] for f in range(num_dp)])
            for plane, at in ((far, 0), (mirror, num_dp))
        )
        arrived[slots * 2 + my_slot] = pooled[me]
        wait_blocks(slots, slots * 2 - 1, 0)
        item_pre = crossed + project(
            (plane, [arrived[at + f] + arrived[at + num_dp + f] for f in range(num_dp)])
            for plane, at in ((near, slots), (c, slots * 2))
        )
    else:
        arrived[me] = pooled[me]
        wait_blocks(0, total - 1, 0)

        def table_block(f):
            block = arrived[f]
            for s in range(1, num_tab):
                block = block + arrived[s * groups + f]
            return block

        item_pre = project(
            (plane, [table_block(plane * num_dp + f) for f in range(num_dp)])
            for plane in range(num_cand)
        )
    item_emb = unit_rows(item_pre)
    emb_out[...] = item_emb

    @pl.loop(0, slots - 1)
    def _(k):
        slot = plane_slot(k) if paired else lax.rem(my_slot + 1 + k, slots)
        pltpu.make_async_remote_copy(
            src_ref=emb_out,
            dst_ref=gathered.at[my_slot],
            send_sem=send_b,
            recv_sem=recv_b,
            device_id=in_plane(slot),
            device_id_type=MESH,
        ).start()

    gathered[my_slot] = item_emb
    pl.loop(early, tiles)(tower)
    others_b = pl.ds(0, slots - 1)
    pltpu.make_async_copy(gathered.at[others_b], gathered.at[others_b], recv_b).wait()
    for s in range(slots):
        items_flat[s * per_block : (s + 1) * per_block, :] = gathered[s]
    item_hi, item_lo = split2(items_flat[...])
    count = slots * per_block
    column = min(users, COLUMN)

    line = lax.broadcasted_iota(jnp.int32, (count, 1), 0)
    slot = line // per_block
    ids = ((slot // num_dp * num_cand + c) * num_dp + slot % num_dp) * per_block + line % per_block

    @pl.loop(0, users // column)
    def _(u):
        rows = pl.ds(pl.multiple_of(u * column, column), column)
        uh, ul = user_hi[rows, :], user_lo[rows, :]

        def cross(a, b):
            return lax.dot_general(a, b, (((1,), (1,)), ((), ())), preferred_element_type=F32)

        scores = cross(item_lo, uh) + cross(item_hi, ul) + cross(item_hi, uh)
        sums_here[0:1, rows] = jnp.sum(jnp.exp2(scores), axis=0, keepdims=True)
        sums_here[1:2, rows] = jnp.sum(
            jnp.where(ids == positives[:, rows], scores, jnp.float32(0.0)), axis=0, keepdims=True
        )

    for j in range(1, num_cand):
        peer = (mirror, far, near)[j - 1] if num_cand == 4 else lax.rem(c + j, num_cand)
        pltpu.make_async_remote_copy(
            src_ref=sums_here,
            dst_ref=sums_all.at[c],
            send_sem=send_c,
            recv_sem=recv_c,
            device_id=(t, peer, d),
            device_id_type=MESH,
        ).start()

    sums_all[c] = sums_here[...]
    others_c = pl.ds(0, num_cand - 1)
    pltpu.make_async_copy(sums_all.at[others_c], sums_all.at[others_c], recv_c).wait()
    both = sums_all[0]
    for s in range(1, num_cand):
        both = both + sums_all[s]
    loss_out[...] = jnp.log(both[0:1, :]) - both[1:2, :] * math.log(2.0)

    pltpu.make_async_copy(pooled.at[others], pooled.at[others], send_a).wait()
    pltpu.make_async_copy(gathered.at[others_b], gathered.at[others_b], send_b).wait()
    pltpu.make_async_copy(sums_all.at[others_c], sums_all.at[others_c], send_c).wait()


TILE = 512
EARLY = 2
AT_ONCE = 2
GAP = 2
COLUMN = 2048


def keep(emb_in, loss_in, emb_out, loss_out, sems):
    pairs = ((emb_in, emb_out), (loss_in, loss_out))
    copies = [pltpu.make_async_copy(a, b, sems.at[i]) for i, (a, b) in enumerate(pairs)]
    for copy in copies:
        copy.start()
    for copy in copies:
        copy.wait()


def body(
    tables, bag_ids, bag_lengths, item_weight, user_features, user_w1, user_w2, positive_items
):
    sizes = tuple(lax.axis_size(n) for n in ("tab", "cand", "dp"))
    total = math.prod(sizes)
    slots = sizes[0] * sizes[2]
    table = tables[0]
    rows, width = table.shape
    items, length = bag_ids.shape[1:]
    per_block = items // total
    users = user_features.shape[0]
    embed = user_w2.shape[1]
    chunk = min(rows, 4096)
    chunks = rows // chunk
    held = min(chunks, 8)
    anywhere = pl.BlockSpec(memory_space=pl.ANY)
    near = pl.BlockSpec(memory_space=pltpu.VMEM)
    item_emb, loss = pl.pallas_call(
        functools.partial(run_step, sizes),
        out_shape=(
            pltpu.VMEM((per_block, embed), F32),
            pltpu.VMEM((1, users), F32),
        ),
        in_specs=[anywhere] * 8,
        out_specs=(near, near),
        scratch_shapes=[
            pltpu.VMEM((length, items), jnp.int32),
            pltpu.VMEM((1, items), jnp.int32),
            pltpu.VMEM((length, items), jnp.int32),
            pltpu.VMEM((items, LANES), F32),
            pltpu.VMEM((held, chunk, width), BF16),
            pltpu.VMEM((rows + ZERO_ROWS, width), F32),
            pltpu.VMEM(item_weight.shape, BF16),
            pltpu.VMEM(user_features.shape, BF16),
            pltpu.VMEM(user_w1.shape, BF16),
            pltpu.VMEM(user_w2.shape, BF16),
            pltpu.VMEM((1, users), jnp.int32),
            pltpu.VMEM((total, per_block, width), F32),
            pltpu.VMEM((total, per_block, width), F32),
            pltpu.VMEM((slots + 1, per_block, width), F32),
            pltpu.VMEM((users, embed), BF16),
            pltpu.VMEM((users, embed), BF16),
            pltpu.VMEM((slots, per_block, embed), F32),
            pltpu.VMEM((slots * per_block, embed), F32),
            pltpu.VMEM((2, users), F32),
            pltpu.VMEM((sizes[1], 2, users), F32),
            pltpu.SemaphoreType.DMA((7,)),
            pltpu.SemaphoreType.DMA((chunks,)),
            pltpu.SemaphoreType.DMA((length,)),
        ]
        + [pltpu.SemaphoreType.DMA, pltpu.SemaphoreType.DMA((2,))]
        + [pltpu.SemaphoreType.DMA] * 4
        + [pltpu.SemaphoreType.REGULAR, pltpu.SemaphoreType.DMA((slots,))]
        + [pltpu.SMEM((items,), jnp.int32)] * length,
        compiler_params=pltpu.CompilerParams(
            collective_id=0, has_side_effects=True, vmem_limit_bytes=VMEM_LIMIT
        ),
        name="step",
    )(
        bag_ids[0].T,
        bag_lengths,
        table,
        item_weight,
        user_features,
        user_w1,
        user_w2,
        positive_items[None, :],
    )
    item_emb, loss = pl.pallas_call(
        keep,
        out_shape=(
            jax.ShapeDtypeStruct((per_block, embed), F32),
            jax.ShapeDtypeStruct((1, users), F32),
        ),
        in_specs=[pl.BlockSpec(memory_space=pltpu.VMEM)] * 2,
        out_specs=(anywhere, anywhere),
        scratch_shapes=[pltpu.SemaphoreType.DMA((2,))],
        name="keep",
    )(*[pltpu.with_memory_space_constraint(x, pltpu.VMEM) for x in (item_emb, loss)])
    return (item_emb, loss[0])


def solution(mesh):
    placed = (
        P(("cand", "dp"), "tab", None),
        P(("cand", "dp"), None, None),
        P(("cand", "dp"), None),
        P(),
        P(("tab", "dp"), None),
        P(),
        P(),
        P(("tab", "dp")),
    )
    return jax.shard_map(
        body,
        mesh=mesh,
        in_specs=placed,
        out_specs=(P(("tab", "cand", "dp"), None), P(("tab", "dp"))),
        check_vma=False,
    )
```

```python
import functools
import math

import jax
import jax.numpy as jnp
from jax import lax
from jax.experimental import pallas as pl
from jax.experimental.pallas import tpu as pltpu
from jax.sharding import PartitionSpec as P

epsilon = 1e-06
logit_scale = 20.0
MESH = pl.DeviceIdType.MESH
F32 = jnp.float32
BF16 = jnp.bfloat16
VMEM_LIMIT = 60 * 1024 * 1024
LANES = 128
SUBLANES = 8
ZERO_ROWS = 32


def split2(x):
    hi = x.astype(BF16)
    return hi, (x - hi.astype(F32)).astype(BF16)


def unit_rows(vectors):
    return vectors * lax.rsqrt(jnp.mean(vectors * vectors, axis=-1, keepdims=True) + epsilon)


def dot(a, b):
    return jnp.dot(a, b, preferred_element_type=F32)


def run_step(
    sizes,
    ids_in,
    lengths_in,
    table,
    weight_in,
    features_in,
    w1_in,
    w2_in,
    positives_in,
    emb_out,
    loss_out,
    ids_raw,
    lengths,
    index_rows,
    inverse,
    narrow,
    wide,
    weight,
    features,
    w1,
    w2,
    positives,
    pooled,
    arrived,
    helped,
    user_hi,
    user_lo,
    gathered,
    items_flat,
    sums_here,
    sums_all,
    load_sems,
    table_sems,
    index_sems,
    send_a,
    recv_a,
    send_b,
    recv_b,
    send_c,
    recv_c,
    ready,
    recv_x,
    *index,
):
    num_tab, num_cand, num_dp = sizes
    total = num_tab * num_cand * num_dp
    groups = num_cand * num_dp
    slots = num_tab * num_dp
    t, c, d = (lax.axis_index(n) for n in ("tab", "cand", "dp"))
    me = (t * num_cand + c) * num_dp + d
    my_slot = t * num_dp + d
    per_block, width = pooled.shape[1:]
    items = total * per_block
    length = ids_raw.shape[0]
    rows, _ = table.shape
    users = features.shape[0]
    hidden = w1.shape[1]
    embed = w2.shape[1]
    chunks = table_sems.shape[0]
    chunk = rows // chunks
    held = narrow.shape[0]
    blocks_step = max(1, 32 // per_block)
    steps = total // blocks_step
    items_step = items // steps
    columns = items // LANES

    paired = num_tab == 2 and num_cand == 4 and num_dp == 4 and blocks_step == 1
    given_end = slots
    kept_start = slots + GAP
    kept_end = kept_start + slots
    far = lax.rem(c + lax.div(num_cand, 2), num_cand)
    mirror = num_cand - 1 - c
    near = c + 1 - 2 * lax.rem(c, 2)

    def place(index):
        return (
            lax.div(index, groups),
            lax.rem(lax.div(index, num_dp), num_cand),
            lax.rem(index, num_dp),
        )

    barrier = pltpu.get_barrier_semaphore()

    loads = [
        pltpu.make_async_copy(a, b, load_sems.at[i])
        for i, (a, b) in enumerate(
            (
                (ids_in, ids_raw),
                (lengths_in, lengths),
                (w1_in, w1),
                (w2_in, w2),
                (features_in, features),
                (weight_in, weight),
                (positives_in, positives),
            )
        )
    ]

    def chunk_copy(n):
        part = pl.ds(pl.multiple_of(n * chunk, chunk), chunk)
        return pltpu.make_async_copy(table.at[part], narrow.at[lax.rem(n, held)], table_sems.at[n])

    def in_plane(slot):
        return (lax.div(slot, num_dp), c, lax.rem(slot, num_dp))

    for load in loads[:2]:
        load.start()

    @pl.loop(1, num_cand)
    def _(j):
        peer = (t, lax.rem(c + j, num_cand), d)
        pl.semaphore_signal(barrier, inc=1, device_id=peer, device_id_type=MESH)

    for n in range(min(chunks, held)):
        chunk_copy(n).start()

    @pl.loop(1, slots)
    def _(j):
        peer = in_plane(lax.rem(my_slot + j, slots))
        pl.semaphore_signal(barrier, inc=1, device_id=peer, device_id_type=MESH)

    helped[slots] = jnp.zeros(helped.shape[1:], F32)
    wide[pl.ds(rows, ZERO_ROWS), :] = jnp.zeros((ZERO_ROWS, width), F32)
    for load in loads[:2]:
        load.wait()
    first_row = t * rows
    spread = lax.broadcasted_iota(jnp.int32, (SUBLANES, LANES), 1) % 2 * (ZERO_ROWS // 2)
    line = lax.broadcasted_iota(jnp.int32, (SUBLANES, LANES), 0)
    for b in range(columns):
        lanes = slice(b * LANES, (b + 1) * LANES)
        count = lengths[:, lanes]
        for p in range(0, length, SUBLANES):
            local = ids_raw[p : p + SUBLANES, lanes] - first_row
            position = line + p
            keeping = (local >= 0) & (local < rows) & (position < count)
            spare = rows + position % (ZERO_ROWS // 2) + spread
            index_rows[p : p + SUBLANES, lanes] = jnp.where(keeping, local, spare)
    index_copies = [
        pltpu.make_async_copy(index_rows.at[p], index[p], index_sems.at[p]) for p in range(length)
    ]
    for copy in index_copies:
        copy.start()
    for b in range(columns):
        lanes = slice(b * LANES, (b + 1) * LANES)
        scale = 1.0 / lengths[:, lanes].astype(F32)
        inverse[lanes, :] = jnp.broadcast_to(scale, (LANES, LANES)).T

    pl.semaphore_wait(barrier, num_cand - 1 + slots - 1)

    @pl.loop(1, slots)
    def _(j):
        peer = in_plane(lax.rem(my_slot + j, slots))
        pl.semaphore_signal(ready, inc=1, device_id=peer, device_id_type=MESH)

    @pl.loop(0, chunks)
    def _(n):
        chunk_copy(n).wait()
        part = pl.ds(pl.multiple_of(n * chunk, chunk), chunk)
        wide[part, :] = narrow[lax.rem(n, held)].astype(F32)
        if held < chunks:

            @pl.when(n + held < chunks)
            def _():
                chunk_copy(n + held).start()

    for load in loads[2:]:
        load.start()
    for copy in index_copies:
        copy.wait()

    def send(dest, slot):
        pltpu.make_async_remote_copy(
            src_ref=pooled.at[dest],
            dst_ref=arrived.at[slot],
            send_sem=send_a,
            recv_sem=recv_a.at[0],
            device_id=place(dest),
            device_id_type=MESH,
        ).start()

    def plane_slot(k):
        outer = k < num_tab
        inner = k >= num_tab + num_dp
        even = lax.rem(k, 2) == 0
        over_tab = outer | (even & ~inner)
        over_row = outer | (~even & ~inner)
        shift = jnp.where(outer | inner, k + 1, lax.div(k, 2))
        tab = jnp.where(over_tab, 1 - t, t)
        row = lax.div(d, 2)
        row = jnp.where(over_row, 1 - row, row)
        return tab * num_dp + row * 2 + lax.rem(d + shift, 2)

    def block_at(s):
        if not paired:
            group = lax.rem(lax.div(me, blocks_step) + 1 + s, steps)
            return (group,)
        i = jnp.where(s < given_end, s, s - kept_start)
        j = s - jnp.where(s < kept_start, given_end, slots * 2)
        close = plane_slot(lax.rem(j, slots))
        crossing = (s < given_end) | ((s >= kept_start) & (s < kept_end))
        tab = jnp.where(
            crossing, jnp.where(s < given_end, 1 - t, t), lax.div(close, num_dp)
        )
        dp = lax.rem(jnp.where(crossing, d + 1 + i, close), num_dp)
        plane = jnp.where(
            crossing,
            jnp.where(i < num_dp, far, mirror),
            jnp.where(j < slots, near, c),
        )
        kept = jnp.where(i < num_dp, 0, num_dp) + d
        direct = jnp.where(j < slots, slots, slots * 2) + my_slot
        target = jnp.where(crossing, jnp.where(s < given_end, i, kept), direct)
        return ((tab * num_cand + plane) * num_dp + dp, tab, plane, dp, target)

    def send_block(s, block, given):
        if not paired:
            for i in range(blocks_step):
                send(block[0] * blocks_step + i, me)
            return
        group, tab, plane, dp, target = block
        if given:
            arrival = helped.at[target], recv_x.at[target], (1 - t, c, d)
        else:
            keeps = (s >= kept_start) & (s < kept_end)
            arrival = arrived.at[target], recv_a.at[jnp.where(keeps, 1, 0)], (tab, plane, dp)
        pltpu.make_async_remote_copy(
            src_ref=pooled.at[group],
            dst_ref=arrival[0],
            send_sem=send_a,
            recv_sem=arrival[1],
            device_id=arrival[2],
            device_id_type=MESH,
        ).start()

    def gather(s, groups_then_now):
        before, groups_now = groups_then_now

        def sends(given):
            for i in range(AT_ONCE):
                send_block(s * AT_ONCE - AT_ONCE + i, before[i], given)

        if paired:

            @pl.when((s > 0) & (s * AT_ONCE <= given_end))
            def _():
                @pl.when(s == 1)
                def _():
                    pl.semaphore_wait(ready, slots - 1)

                sends(True)

            @pl.when(s * AT_ONCE > given_end)
            def _():
                sends(False)

            @pl.when((s * AT_ONCE >= kept_start) & (s * AT_ONCE < kept_end))
            def _():
                for i in range(AT_ONCE):
                    at = s * AT_ONCE + i - kept_start
                    block = helped.at[at]
                    pltpu.make_async_copy(block, block, recv_x.at[at]).wait()
        else:

            @pl.when(s > 0)
            def _():
                @pl.when(s == 1)
                def _():
                    pl.semaphore_wait(ready, slots - 1)

                sends(False)

        for i in range(AT_ONCE):
            now = s * AT_ONCE + i
            group = groups_now[i][0]
            first = group * items_step
            if paired:
                keeps = (now >= kept_start) & (now < kept_end)
                help_at = jnp.where(keeps, now - kept_start, slots)
            for k in range(items_step):
                terms = [wide[pl.ds(of_place[first + k], 1), :] for of_place in index]
                while len(terms) > 1:
                    terms = [a + b for a, b in zip(terms[::2], terms[1::2])] + (
                        [terms[-1]] if len(terms) % 2 else []
                    )
                row = terms[0] * inverse[pl.ds(first + k, 1), :]
                if paired:
                    row = row + helped[help_at, pl.ds(k, 1), :]
                pooled[group * blocks_step + k // per_block, pl.ds(k % per_block, 1), :] = row

        return groups_now, groups_of(s + 1)

    def groups_of(s):
        return tuple(block_at(s * AT_ONCE + i) for i in range(AT_ONCE))

    start = groups_of(jnp.int32(0))
    finish, _ = lax.fori_loop(0, steps // AT_ONCE, gather, (start, start))
    for i in range(AT_ONCE - 1):
        send_block(jnp.int32(steps - AT_ONCE + i), finish[i], False)
    last = finish[AT_ONCE - 1][0]
    for i in range(blocks_step):
        dest = last * blocks_step + i
        if blocks_step > 1:

            @pl.when(dest != me)
            def _():
                send(dest, me)

    for load in loads[2:]:
        load.wait()
    tile = min(users, TILE)
    part_width = min(hidden, 256)

    def tower(n):
        user_rows = pl.ds(pl.multiple_of(n * tile, tile), tile)
        x = features[user_rows, :]
        pre = None
        for h in range(0, hidden, part_width):
            z = dot(x, w1[:, h : h + part_width])
            z = z * lax.erf(z * math.sqrt(0.5)) + z
            term = dot(z.astype(BF16), w2[h : h + part_width, :])
            pre = term if pre is None else pre + term
        hi, lo = split2(unit_rows(pre * 0.5) * (logit_scale / embed * math.log2(math.e)))
        user_hi[user_rows, :] = hi
        user_lo[user_rows, :] = lo

    tiles = users // tile
    early = tiles * EARLY // 8
    pl.loop(0, early)(tower)

    others = pl.ds(0, total - 1)

    def wait_blocks(first, number, kind):
        blocks = arrived.at[pl.ds(first, number)]
        pltpu.make_async_copy(blocks, blocks, recv_a.at[kind]).wait()

    def project(planes):
        depth = num_dp * width
        result = None
        for plane, blocks in planes:
            part = jnp.concatenate(split2(jnp.concatenate(blocks, axis=1)), axis=0)
            at = pl.ds(pl.multiple_of(plane * depth, depth), depth)
            term = dot(part, weight[at, :])
            result = term if result is None else result + term
        return result[:per_block] + result[per_block:]

    if paired:
        wait_blocks(0, slots, 1)
        crossed = project(
            (plane, [arrived[at + f] for f in range(num_dp)])
            for plane, at in ((far, 0), (mirror, num_dp))
        )
        arrived[slots * 2 + my_slot] = pooled[me]
        wait_blocks(slots, slots * 2 - 1, 0)
        item_pre = crossed + project(
            (plane, [arrived[at + f] + arrived[at + num_dp + f] for f in range(num_dp)])
            for plane, at in ((near, slots), (c, slots * 2))
        )
    else:
        arrived[me] = pooled[me]
        wait_blocks(0, total - 1, 0)

        def table_block(f):
            block = arrived[f]
            for s in range(1, num_tab):
                block = block + arrived[s * groups + f]
            return block

        item_pre = project(
            (plane, [table_block(plane * num_dp + f) for f in range(num_dp)])
            for plane in range(num_cand)
        )
    item_emb = unit_rows(item_pre)
    emb_out[...] = item_emb

    @pl.loop(0, slots - 1)
    def _(k):
        slot = plane_slot(k) if paired else lax.rem(my_slot + 1 + k, slots)
        pltpu.make_async_remote_copy(
            src_ref=emb_out,
            dst_ref=gathered.at[my_slot],
            send_sem=send_b,
            recv_sem=recv_b,
            device_id=in_plane(slot),
            device_id_type=MESH,
        ).start()

    gathered[my_slot] = item_emb
    pl.loop(early, tiles)(tower)
    others_b = pl.ds(0, slots - 1)
    pltpu.make_async_copy(gathered.at[others_b], gathered.at[others_b], recv_b).wait()
    for s in range(slots):
        items_flat[s * per_block : (s + 1) * per_block, :] = gathered[s]
    item_hi, item_lo = split2(items_flat[...])
    count = slots * per_block
    column = min(users, COLUMN)

    line = lax.broadcasted_iota(jnp.int32, (count, 1), 0)
    slot = line // per_block
    ids = ((slot // num_dp * num_cand + c) * num_dp + slot % num_dp) * per_block + line % per_block

    @pl.loop(0, users // column)
    def _(u):
        rows = pl.ds(pl.multiple_of(u * column, column), column)
        uh, ul = user_hi[rows, :], user_lo[rows, :]

        def cross(a, b):
            return lax.dot_general(a, b, (((1,), (1,)), ((), ())), preferred_element_type=F32)

        scores = cross(item_lo, uh) + cross(item_hi, ul) + cross(item_hi, uh)
        sums_here[0:1, rows] = jnp.sum(jnp.exp2(scores), axis=0, keepdims=True)
        sums_here[1:2, rows] = jnp.sum(
            jnp.where(ids == positives[:, rows], scores, jnp.float32(0.0)), axis=0, keepdims=True
        )

    for j in range(1, num_cand):
        peer = (mirror, far, near)[j - 1] if num_cand == 4 else lax.rem(c + j, num_cand)
        pltpu.make_async_remote_copy(
            src_ref=sums_here,
            dst_ref=sums_all.at[c],
            send_sem=send_c,
            recv_sem=recv_c,
            device_id=(t, peer, d),
            device_id_type=MESH,
        ).start()

    sums_all[c] = sums_here[...]
    others_c = pl.ds(0, num_cand - 1)
    pltpu.make_async_copy(sums_all.at[others_c], sums_all.at[others_c], recv_c).wait()
    both = sums_all[0]
    for s in range(1, num_cand):
        both = both + sums_all[s]
    loss_out[...] = jnp.log(both[0:1, :]) - both[1:2, :] * math.log(2.0)

    pltpu.make_async_copy(pooled.at[others], pooled.at[others], send_a).wait()
    pltpu.make_async_copy(gathered.at[others_b], gathered.at[others_b], send_b).wait()
    pltpu.make_async_copy(sums_all.at[others_c], sums_all.at[others_c], send_c).wait()


TILE = 512
EARLY = 2
AT_ONCE = 2
GAP = 6
COLUMN = 2048


def keep(emb_in, loss_in, emb_out, loss_out, sems):
    pairs = ((emb_in, emb_out), (loss_in, loss_out))
    copies = [pltpu.make_async_copy(a, b, sems.at[i]) for i, (a, b) in enumerate(pairs)]
    for copy in copies:
        copy.start()
    for copy in copies:
        copy.wait()


def body(
    tables, bag_ids, bag_lengths, item_weight, user_features, user_w1, user_w2, positive_items
):
    sizes = tuple(lax.axis_size(n) for n in ("tab", "cand", "dp"))
    total = math.prod(sizes)
    slots = sizes[0] * sizes[2]
    table = tables[0]
    rows, width = table.shape
    items, length = bag_ids.shape[1:]
    per_block = items // total
    users = user_features.shape[0]
    embed = user_w2.shape[1]
    chunk = min(rows, 4096)
    chunks = rows // chunk
    held = min(chunks, 8)
    anywhere = pl.BlockSpec(memory_space=pl.ANY)
    near = pl.BlockSpec(memory_space=pltpu.VMEM)
    item_emb, loss = pl.pallas_call(
        functools.partial(run_step, sizes),
        out_shape=(
            pltpu.VMEM((per_block, embed), F32),
            pltpu.VMEM((1, users), F32),
        ),
        in_specs=[anywhere] * 8,
        out_specs=(near, near),
        scratch_shapes=[
            pltpu.VMEM((length, items), jnp.int32),
            pltpu.VMEM((1, items), jnp.int32),
            pltpu.VMEM((length, items), jnp.int32),
            pltpu.VMEM((items, LANES), F32),
            pltpu.VMEM((held, chunk, width), BF16),
            pltpu.VMEM((rows + ZERO_ROWS, width), F32),
            pltpu.VMEM(item_weight.shape, BF16),
            pltpu.VMEM(user_features.shape, BF16),
            pltpu.VMEM(user_w1.shape, BF16),
            pltpu.VMEM(user_w2.shape, BF16),
            pltpu.VMEM((1, users), jnp.int32),
            pltpu.VMEM((total, per_block, width), F32),
            pltpu.VMEM((total, per_block, width), F32),
            pltpu.VMEM((slots + 1, per_block, width), F32),
            pltpu.VMEM((users, embed), BF16),
            pltpu.VMEM((users, embed), BF16),
            pltpu.VMEM((slots, per_block, embed), F32),
            pltpu.VMEM((slots * per_block, embed), F32),
            pltpu.VMEM((2, users), F32),
            pltpu.VMEM((sizes[1], 2, users), F32),
            pltpu.SemaphoreType.DMA((7,)),
            pltpu.SemaphoreType.DMA((chunks,)),
            pltpu.SemaphoreType.DMA((length,)),
        ]
        + [pltpu.SemaphoreType.DMA, pltpu.SemaphoreType.DMA((2,))]
        + [pltpu.SemaphoreType.DMA] * 4
        + [pltpu.SemaphoreType.REGULAR, pltpu.SemaphoreType.DMA((slots,))]
        + [pltpu.SMEM((items,), jnp.int32)] * length,
        compiler_params=pltpu.CompilerParams(
            collective_id=0, has_side_effects=True, vmem_limit_bytes=VMEM_LIMIT
        ),
        name="step",
    )(
        bag_ids[0].T,
        bag_lengths,
        table,
        item_weight,
        user_features,
        user_w1,
        user_w2,
        positive_items[None, :],
    )
    item_emb, loss = pl.pallas_call(
        keep,
        out_shape=(
            jax.ShapeDtypeStruct((per_block, embed), F32),
            jax.ShapeDtypeStruct((1, users), F32),
        ),
        in_specs=[pl.BlockSpec(memory_space=pltpu.VMEM)] * 2,
        out_specs=(anywhere, anywhere),
        scratch_shapes=[pltpu.SemaphoreType.DMA((2,))],
        name="keep",
    )(*[pltpu.with_memory_space_constraint(x, pltpu.VMEM) for x in (item_emb, loss)])
    return (item_emb, loss[0])


def solution(mesh):
    placed = (
        P(("cand", "dp"), "tab", None),
        P(("cand", "dp"), None, None),
        P(("cand", "dp"), None),
        P(),
        P(("tab", "dp"), None),
        P(),
        P(),
        P(("tab", "dp")),
    )
    return jax.shard_map(
        body,
        mesh=mesh,
        in_specs=placed,
        out_specs=(P(("tab", "cand", "dp"), None), P(("tab", "dp"))),
        check_vma=False,
    )
```
